32 devices in a mesh: gx: 16 (over z, x, core), gy: 2 (over y).
Axes of the slice: x: 2, y: 2, z: 4, core: 2. Of those that a mesh axis runs over, the one named last changes fastest.
Arguments:
- voltage: float32 [256, 64, 128], P('gx', 'gy'), may hold values from -0.5 to 1.5
- potential: float32 [256, 64, 128], P('gx', 'gy'), may hold values from -6 to 6
- tissue: int32 [256, 64, 128], P('gx', 'gy'), may hold values 0 or 1
- gain: float32 [256, 64, 128], P('gx', 'gy'), may hold values from 0.25 to 1.75
- couplings: float32 [2, 9], replicated, may hold values from 0.05 to 0.5
- line_factor: float32 [256, 256], replicated, as said below
Outputs:
- new_voltage: float32 [256, 64, 128], P('gx', 'gy')
- new_potential: float32 [256, 64, 128], P('gx', 'gy')
The draws below stay inside these ranges and needn't reach their ends.
Inputs may be any that keep to these rules, and one draw needn't show every extreme that they name: line_factor is lower triangular with positive diagonal entries.
All inputs are finite; a program needn't handle non-finite values. No bound on the sum of `tissue` on one device may be relied on, other than what follows from the above.
Results may differ from the reference program's by a relative error of at most 0.0003.
Values sent between devices are 32-bit elements; how exact they have to be, the bound alone decides.
No kernel may reach another device: no remote copies, remote signals or barrier semaphores. Data moves between devices by JAX's collectives and lax.ppermute only.
A program may use at most 64 MiB of HBM per device.

```python
import math
import jax
import jax.numpy as jnp
from jax import lax

NX = 128
NZ = 256
CHEB = 8
ITERS = 4
NY = 64


def draw_line_factor(key, part):
    diag_key = jax.random.fold_in(key, 11)
    rest_key = jax.random.fold_in(key, 12)
    diag_vals = jax.random.uniform(diag_key, (NZ,), jnp.float32, 1.0, 2.0)
    off_scale = 0.35
    lower = jnp.tril(jax.random.normal(rest_key, (NZ, NZ), jnp.float32), -1) * (off_scale / math.sqrt(NZ))
    return lower + jnp.diag(diag_vals)


def with_ends(array, own_key, least, top_value):
    shape = array.shape
    spot = [jax.random.randint(jax.random.fold_in(own_key, axis), (), 0, shape[axis]) for axis in range(len(shape))]
    array = array.at[tuple(spot)].set(least)
    longest = shape.index(max(shape))
    spot[longest] = (spot[longest] + 1) % shape[longest]
    return array.at[tuple(spot)].set(top_value)


def block_scale(own_key, shape, split, low, top_value):
    level, own = 1.0, jax.random.fold_in(own_key, 6)
    for axis_at, blocks in split:
        draws = jnp.exp(jax.random.uniform(jax.random.fold_in(own, axis_at), (blocks,), jnp.float32, low / len(split), top_value / len(split)))
        level = level * jnp.repeat(draws, shape[axis_at] // blocks).reshape([-1 if axis == axis_at else 1 for axis in range(len(shape))])
    return level


def bell_draw(stream_key, shape, width, reach, split=(), dtype=jnp.bfloat16):
    values = jax.random.normal(stream_key, shape, jnp.float32) * width
    if len(split) > 0:
        values = block_scale(stream_key, shape, split, -0.22, 0.18) * values
    return jnp.clip(values, min=-reach, max=reach).astype(dtype)


def setup_inputs(seed: int = 0) -> dict:
    splits = jax.random.split(jax.random.key(seed), 7)
    voltage = jnp.clip(-0.5 + 2.0 * jax.random.uniform(splits[0], (NZ, NY, NX), jnp.float32) ** block_scale(splits[0], (NZ, NY, NX), ((0, 16), (1, 2)), -0.2, 0.2), -0.5, 1.5)
    potential = bell_draw(splits[1], (NZ, NY, NX), 1.0, 6.0, ((0, 16), (1, 2)), jnp.float32)
    tissue = with_ends((jax.random.randint(splits[2], (NZ, NY, NX), 0, 4) < 3).astype(jnp.int32), jax.random.fold_in(splits[2], 1), 0, 1)
    gain = jnp.clip(1.0 + 0.15 * jax.random.normal(splits[3], (NZ, NY, NX), jnp.float32), 0.25, 1.75)
    couplings = jnp.clip(jnp.exp(jax.random.uniform(splits[4], (2, 9), jnp.float32, math.log(0.05), math.log(0.5))), 0.05, 0.5)
    line_factor = draw_line_factor(jax.random.fold_in(splits[6], 71), 0)
    return dict(voltage=voltage, potential=potential, tissue=tissue, gain=gain, couplings=couplings, line_factor=line_factor)


highest = lax.Precision.HIGHEST
time_step = 2.0
ionic_rate = 0.5
onset_level = 0.2
gain_top = 3.0625
neighbours = ((1, 0, 0, 0), (-1, 0, 0, 0), (0, 1, 0, 1), (0, -1, 0, 1), (0, 0, 1, 2), (0, 0, -1, 2),
              (1, 1, 0, 3), (-1, -1, 0, 3), (1, -1, 0, 4), (-1, 1, 0, 4), (1, 0, 1, 5), (-1, 0, -1, 5),
              (1, 0, -1, 6), (-1, 0, 1, 6), (0, 1, 1, 7), (0, -1, -1, 7), (0, 1, -1, 8), (0, -1, 1, 8))


def shifted(padded, move_z, move_y, move_x):
    extent_z, extent_y, extent_x = padded.shape
    return padded[1 + move_z:extent_z - 1 + move_z, 1 + move_y:extent_y - 1 + move_y, 1 + move_x:extent_x - 1 + move_x]


def fluxes(vector_pad, cond_pad, intra_coef, extra_coef):
    centre = shifted(vector_pad, 0, 0, 0)
    intra = jnp.zeros_like(centre)
    extra = jnp.zeros_like(centre)
    for move_z, move_y, move_x, column in neighbours:
        difference = centre - shifted(vector_pad, move_z, move_y, move_x)
        intra = intra + intra_coef[column] * shifted(cond_pad, move_z, move_y, move_x) * difference
        extra = extra + extra_coef[column] * difference
    return shifted(cond_pad, 0, 0, 0) * intra, extra


def along_lines(vector, line_factor):
    extent = vector.shape
    matrix = vector.reshape(extent[0], -1)
    first = jnp.dot(line_factor, matrix, precision=highest)
    second = jnp.dot(line_factor.T, first, precision=highest)
    return second.reshape(extent)


def reference(voltage, potential, tissue, gain, couplings, line_factor):
    mask_f = tissue.astype(jnp.float32)
    conduct = mask_f * gain
    cond_pad = jnp.pad(conduct, 1)
    intra_coef = couplings[0]
    extra_coef = couplings[1]
    volt_intra, volt_extra = fluxes(jnp.pad(voltage, 1), cond_pad, intra_coef, extra_coef)
    pot_intra, pot_extra = fluxes(jnp.pad(potential, 1), cond_pad, intra_coef, extra_coef)
    ionic = mask_f * voltage * (voltage - onset_level) * (voltage - 1.0)
    source = voltage - ionic_rate * ionic - time_step * pot_intra
    residual = source - (voltage + time_step * volt_intra)
    top_eig = 1.0 + time_step * 4.0 * gain_top * jnp.sum(intra_coef)
    centre_eig = (top_eig + 1.0) / 2.0
    half_width = (top_eig - 1.0) / 2.0
    spread_ratio = centre_eig / half_width
    weight_now = 1.0 / spread_ratio
    update = residual / centre_eig
    estimate = voltage
    for sweep in range(CHEB):
        estimate = estimate + update
        if sweep < CHEB - 1:
            upd_intra, upd_extra = fluxes(jnp.pad(update, 1), cond_pad, intra_coef, extra_coef)
            residual = residual - (update + time_step * upd_intra)
            weight_next = 1.0 / (2.0 * spread_ratio - weight_now)
            update = weight_next * weight_now * update + (2.0 * weight_next / half_width) * residual
            weight_now = weight_next
    est_intra, est_extra = fluxes(jnp.pad(estimate, 1), cond_pad, intra_coef, extra_coef)
    residual = -est_intra - (pot_intra + pot_extra)
    approx = potential
    smoothed = along_lines(residual, line_factor)
    search = smoothed
    energy = jnp.sum(residual * smoothed)
    for turn in range(ITERS):
        image_intra, image_extra = fluxes(jnp.pad(search, 1), cond_pad, intra_coef, extra_coef)
        image = image_intra + image_extra
        step_size = energy / jnp.sum(search * image)
        approx = approx + step_size * search
        if turn < ITERS - 1:
            residual = residual - step_size * image
            smoothed = along_lines(residual, line_factor)
            energy_new = jnp.sum(residual * smoothed)
            search = smoothed + (energy_new / energy) * search
            energy = energy_new
    return estimate, approx
```

```python
import jax
import jax.numpy as jnp
from jax import lax
from jax.experimental import pallas as pl
from jax.experimental.pallas import tpu as pltpu
from jax.sharding import PartitionSpec as P

CHEB = 8
ITERS = 4
SUB = 8

time_step = 2.0
ionic_rate = 0.5
onset_level = 0.2
gain_top = 3.0625
f32 = jnp.float32
VMEM = pl.BlockSpec(memory_space=pltpu.VMEM)
SMEM = pl.BlockSpec(memory_space=pltpu.SMEM)


def up_to(n, m):
    return -(-n // m) * m


class Plan:
    def __init__(self, local_shape, ngx, ngy):
        self.nz, self.ny, self.nx = local_shape
        self.ngx, self.ngy = ngx, ngy
        self.depth = ITERS
        self.hz = CHEB + 1
        self.hy = up_to(CHEB + 1 + ITERS, SUB)
        self.swap = ngy == 2
        self.hops = []
        left, hop = self.hz, 1
        while left > 0:
            self.hops.append((hop, min(self.nz, left)))
            left -= self.nz
            hop += 1
        self.pad = up_to(ITERS + 1, SUB)
        self.ywin = self.ny + self.hy * (1 if self.swap else 2)
        self.yrows = self.ywin + 2 * self.pad
        self.zrows = up_to(max(self.hz - d + up_to(self.nz + 2 * d, SUB) + 1 for d in range(self.hz)), SUB)
        self.zrows = max(self.zrows, up_to(self.nz + 2 * self.hz, SUB))
        self.NZ = self.nz * ngx
        self.cols = self.nx // ngx
        self.wid = 1
        while self.wid < self.cols + 2 * self.depth:
            self.wid *= 2
        self.hx = (self.wid - self.cols) // 2
        self.grp = self.nx // self.wid
        self.slabs = -(-(self.ny + 2 * self.depth) // self.grp)
        self.back_grp = self.nx // self.cols
        self.back = self.ny // self.back_grp


def prep_kernel(plan, idx, volt, pot, tissue, gain, cond, *outs):
    cond[...] = tissue[...].astype(f32) * gain[...]
    fields = (volt, pot, cond)
    if plan.swap:
        ys = [pl.multiple_of((1 - idx[1]) * (plan.ny - plan.hy), SUB)]
    else:
        ys = [plan.ny - plan.hy, 0]
    at = 0
    for y0 in ys:
        for f, ref in enumerate(fields):
            outs[at][f] = ref[:, pl.ds(y0, plan.hy), :]
        at += 1
    for _, n in plan.hops:
        for z0 in (plan.nz - n, 0):
            for f, ref in enumerate(fields):
                outs[at][f] = ref[pl.ds(z0, n)]
            at += 1
            for y0 in ys:
                for f, ref in enumerate(fields):
                    outs[at][f] = ref[pl.ds(z0, n), pl.ds(y0, plan.hy), :]
                at += 1


def combine(tile, coef, left, right, width):
    k = coef
    mid, zp, zm, yp, ym = tile(0, 0), tile(1, 0), tile(-1, 0), tile(0, 1), tile(0, -1)
    zpyp, zmym, zpym, zmyp = tile(1, 1), tile(-1, -1), tile(1, -1), tile(-1, 1)
    same = k[0] * (zp + zm) + k[1] * (yp + ym) + k[3] * (zpyp + zmym) + k[4] * (zpym + zmyp)
    face = k[2] * mid
    plus = face + k[5] * zp + k[6] * zm + k[7] * yp + k[8] * ym
    minus = face + k[5] * zm + k[6] * zp + k[7] * ym + k[8] * yp
    plus = pltpu.roll(plus, width - 1, 1)
    minus = pltpu.roll(minus, 1, 1)
    if left is not None:
        plus = jnp.where(right, 0.0, plus)
        minus = jnp.where(left, 0.0, minus)
    return same + plus + minus


def cheb_kernel(plan, idx, coup, volt, pot, cond, *rest):
    p = plan
    ny_halo = 1 if p.swap else 2
    n_in = ny_halo + len(p.hops) * 2 * (1 + ny_halo)
    halos = rest[:n_in]
    new_volt, send = rest[n_in : n_in + 2]
    C, G0, G1, E, PT, R, U, CS = rest[n_in + 2 :]
    nx = p.nx
    flat = lambda ref: ref.reshape(p.yrows * p.zrows, nx)
    if p.swap:
        ylocal = p.pad + idx[1] * p.hy
        yhalo = [p.pad + (1 - idx[1]) * p.ny]
    else:
        ylocal = p.pad + p.hy
        yhalo = [p.pad, p.pad + p.hy + p.ny]

    zero_rows = jnp.zeros((p.pad, p.zrows, nx), f32)
    for ref in (C, G0, G1, E, PT, R):
        ref[pl.ds(0, p.pad)] = zero_rows
        ref[pl.ds(p.pad + p.ywin, p.pad)] = zero_rows

    fc, fg, fe, fp, fr = (flat(r) for r in (C, G0, E, PT, R))

    def place(getter, planes, zrow0, yrow0, ycount):
        def one(z, carry):
            for t in range(ycount // SUB):
                v, q, c = getter(z, t)
                start = (yrow0 + t * SUB) * p.zrows + zrow0 + z
                rows = pl.ds(start, SUB, stride=p.zrows)
                s = v + q
                mask = jnp.where(c > 0.0, 1.0, 0.0)
                fc[rows, :] = c
                fg[rows, :] = c * s
                fe[rows, :] = s
                fp[rows, :] = q
                fr[rows, :] = (-ionic_rate) * mask * v * (v - onset_level) * (v - 1.0)
            return carry

        lax.fori_loop(0, planes, one, 0)

    def local(z, t):
        ys = pl.ds(t * SUB, SUB)
        return volt[z, ys, :], pot[z, ys, :], cond[z, ys, :]

    def piece(ref):
        def get(z, t):
            ys = pl.ds(t * SUB, SUB)
            return ref[0, z, ys, :], ref[1, z, ys, :], ref[2, z, ys, :]

        return get

    place(local, p.nz, p.hz, ylocal, p.ny)
    at = 0
    for y0 in yhalo:
        place(piece(halos[at]), p.nz, p.hz, y0, p.hy)
        at += 1
    done = 0
    for _, n in p.hops:
        for z0 in (p.hz - done - n, p.hz + p.nz + done):
            place(piece(halos[at]), n, z0, ylocal, p.ny)
            at += 1
            for y0 in yhalo:
                place(piece(halos[at]), n, z0, y0, p.hy)
                at += 1
        done += n

    lane = lax.broadcasted_iota(jnp.int32, (SUB, nx), 1)
    left, right = lane == 0, lane == nx - 1
    ki = [coup[0, k] for k in range(9)]
    ke = [coup[1, k] for k in range(9)]

    total = ki[0]
    for k in ki[1:]:
        total = total + k
    top = 1.0 + time_step * 4.0 * gain_top * jnp.full((SUB, nx), total, f32)
    centre = (top + 1.0) / 2.0
    half = (top - 1.0) / 2.0
    ratio = centre / half
    weight = 1.0 / ratio
    inv_centre = 1.0 / centre

    def sweep(d, body):
        tiles = up_to(p.nz + 2 * d, SUB) // SUB
        over = p.hy - p.depth - d
        y0 = p.pad + (idx[1] * over if p.swap else over)
        count = p.ny + (d + p.depth) * (1 if p.swap else 2)

        def row(i, carry):
            y = y0 + i
            for t in range(tiles):
                body(y, p.hz - d + t * SUB)
            return carry

        lax.fori_loop(0, count, row, 0)

    def tile_of(ref, y, z):
        return lambda dz, dy: ref[y + dy, pl.ds(z + dz, SUB), :]

    def first(y, z):
        rows = pl.ds(z, SUB)
        c = C[y, rows, :]
        s = E[y, rows, :]
        cs = c * combine(tile_of(C, y, z), ki, left, right, nx)
        flow = cs * s - c * combine(tile_of(G0, y, z), ki, left, right, nx)
        r = R[y, rows, :] - time_step * flow
        u = r * inv_centre
        CS[y, rows, :] = cs
        R[y, rows, :] = r
        U[y, rows, :] = u
        E[y, rows, :] = s + u
        G1[y, rows, :] = c * u

    sweep(CHEB, first)
    bufs = [G0, G1]
    for k in range(1, CHEB):
        gin, gout = bufs[k % 2], bufs[(k + 1) % 2]
        nxt = 1.0 / (2.0 * ratio - weight)
        keep, add = nxt * weight, 2.0 * nxt / half
        weight = nxt
        last = k == CHEB - 1

        def step(y, z, gin=gin, gout=gout, keep=keep, add=add, last=last):
            rows = pl.ds(z, SUB)
            c = C[y, rows, :]
            u = U[y, rows, :]
            flow = CS[y, rows, :] * u - c * combine(tile_of(gin, y, z), ki, left, right, nx)
            r = R[y, rows, :] - (u + time_step * flow)
            u = keep * u + add * r
            e = E[y, rows, :] + u
            E[y, rows, :] = e
            if last:
                gout[y, rows, :] = c * e
            else:
                R[y, rows, :] = r
                U[y, rows, :] = u
                gout[y, rows, :] = c * u

        sweep(CHEB - k, step)

    gin = bufs[CHEB % 2]
    ke_sum = ke[0]
    for k in ke[1:]:
        ke_sum = ke_sum + k
    ke_sum = 2.0 * ke_sum

    def final(y, z):
        rows = pl.ds(z, SUB)
        c = C[y, rows, :]
        flow = CS[y, rows, :] * E[y, rows, :] - c * combine(tile_of(gin, y, z), ki, left, right, nx)
        outer = ke_sum * PT[y, rows, :] - combine(tile_of(PT, y, z), ke, left, right, nx)
        R[y, rows, :] = -flow - outer

    sweep(0, final)

    def give(z, carry):
        for t in range(p.ny // SUB):
            start = (ylocal + t * SUB) * p.zrows + p.hz + z
            rows = pl.ds(start, SUB, stride=p.zrows)
            new_volt[z, pl.ds(t * SUB, SUB), :] = fe[rows, :] - fp[rows, :]
        return carry

    lax.fori_loop(0, p.nz, give, 0)

    group = lane // p.wid
    first_row = ylocal - p.depth

    def pack(s, carry):
        for f, ref in enumerate((R, C)):
            for zt in range(p.nz // SUB):
                src = [ref[first_row + q * p.slabs + s, pl.ds(p.hz + zt * SUB, SUB), :] for q in range(p.grp)]
                for j in range(p.ngx):
                    acc = None
                    for q in range(p.grp):
                        amount = (p.wid * q - (p.cols * j - p.hx)) % nx
                        part = pltpu.roll(src[q], amount, 1) if amount else src[q]
                        acc = part if acc is None else jnp.where(group == q, part, acc)
                    row = (f * p.slabs + s) * p.nz + zt * SUB
                    send[j, pl.ds(pl.multiple_of(row, SUB), SUB), :] = acc
        return carry

    lax.fori_loop(0, p.slabs, pack, 0)


def factor_kernel(line, line_t, hi, lo, size):
    scale = 1.0 / jnp.max(jnp.abs(line[...]), keepdims=True)
    a = line_t[...] * scale
    b = line[...] * scale
    g = jnp.dot(a, b, precision=lax.Precision.HIGHEST, preferred_element_type=f32)
    high = g.astype(jnp.bfloat16)
    hi[...] = high
    lo[...] = (g - high.astype(f32)).astype(jnp.bfloat16)

    def norm(m):
        return jnp.sqrt(jnp.sum(jnp.sum(m * m, axis=0, keepdims=True), axis=1, keepdims=True))

    n = norm(g)
    est = n
    m = g / n
    for power in range(3):
        mb = m.astype(jnp.bfloat16)
        m = jnp.dot(mb, mb, preferred_element_type=f32)
        n = norm(m)
        m = m / n
        root = n
        for _ in range(power + 1):
            root = jnp.sqrt(root)
        est = est * root
    size[...] = jnp.broadcast_to(est, size.shape)


def basis_kernel(plan, idx, coup, recv, hi, lo, size, basis, sums, C, CS, G, W, B0, B1, B2, BH, BL):
    p = plan
    nx, off = p.nx, SUB
    lane = lax.broadcasted_iota(jnp.int32, (SUB, nx), 1)
    x = p.cols * idx[0] - p.hx + lane % p.wid
    xin = (x >= 0) & (x < nx)
    xown = (lane % p.wid >= p.hx) & (lane % p.wid < p.hx + p.cols)
    ki = [coup[0, k] for k in range(9)]
    ke = [coup[1, k] for k in range(9)]
    ki_sum, ke_sum = ki[0], ke[0]
    for k in range(1, 9):
        ki_sum = ki_sum + ki[k]
        ke_sum = ke_sum + ke[k]
    lam = 2.0 * (ki_sum + ke_sum) * size[...]
    quarter = 4.0 / lam
    ke_twice = 2.0 * ke_sum

    def ywin(s):
        return (lane // p.wid) * p.slabs + s

    def inside(s):
        y = p.ny * idx[1] - p.depth + ywin(s)
        return xin & (y >= 0) & (y < p.ny * p.ngy)

    def own(s):
        return xown & (ywin(s) >= p.depth) & (ywin(s) < p.depth + p.ny)

    for ref in (G, W):
        for s in range(p.slabs + 2):
            ref[s, pl.ds(0, off), :] = jnp.zeros((off, nx), f32)
            ref[s, pl.ds(off + p.NZ, off), :] = jnp.zeros((off, nx), f32)

    zts = p.NZ // SUB
    for s in range(p.slabs):
        keep = inside(s)
        for j in range(p.ngx):
            for zt in range(p.nz // SUB):
                rows = pl.ds(j * p.nz + zt * SUB, SUB)
                B0[s, rows, :] = jnp.where(keep, recv[j, pl.ds(s * p.nz + zt * SUB, SUB), :], 0.0)
                c = jnp.where(keep, recv[j, pl.ds((p.slabs + s) * p.nz + zt * SUB, SUB), :], 0.0)
                C[s, rows, :] = c
                G[s + 1, pl.ds(off + j * p.nz + zt * SUB, SUB), :] = c

    def wrap(ref):
        body = pl.ds(off, p.NZ)
        ref[0, body, :] = pltpu.roll(ref[p.slabs, body, :], p.wid, 1)
        ref[p.slabs + 1, body, :] = pltpu.roll(ref[1, body, :], nx - p.wid, 1)

    wrap(G)

    def tile_of(ref, s, z):
        return lambda dz, dy: ref[s + 1 + dy, pl.ds(off + z + dz, SUB), :]

    for s in range(p.slabs):

        def weigh(t, carry, s=s):
            z = pl.multiple_of(t * SUB, SUB)
            CS[s, pl.ds(z, SUB), :] = C[s, pl.ds(z, SUB), :] * combine(tile_of(G, s, z), ki, None, None, nx)
            return carry

        lax.fori_loop(0, zts, weigh, 0)

    ring = [B0, B1, B2]
    row_id = lax.broadcasted_iota(jnp.int32, (2 * SUB, nx), 0)
    lane_id = lax.broadcasted_iota(jnp.int32, (2 * SUB, nx), 1)
    out = jnp.zeros((1, nx), f32)

    def lane_put(out, acc, at):
        v = jnp.sum(jnp.sum(acc, axis=1, keepdims=True), axis=0, keepdims=True)
        return jnp.where(lax.broadcasted_iota(jnp.int32, (1, nx), 1) == at, v, out)

    zero = jnp.zeros((SUB, nx), f32)
    slot = p.depth
    for j in range(p.depth):
        cur = ring[j % 3]
        prev = ring[(j + 2) % 3]
        new = ring[(j + 1) % 3]
        for s in range(p.slabs):
            b = cur[s]
            high = b.astype(jnp.bfloat16)
            BH[:, pl.ds(s * nx, nx)] = high
            BL[:, pl.ds(s * nx, nx)] = (b - high.astype(f32)).astype(jnp.bfloat16)
        prod = (
            jnp.dot(hi[...], BH[...], preferred_element_type=f32)
            + jnp.dot(hi[...], BL[...], preferred_element_type=f32)
            + jnp.dot(lo[...], BH[...], preferred_element_type=f32)
        )
        for s in range(p.slabs):
            part = prod[:, s * nx : (s + 1) * nx]
            basis[j, s] = part
            W[s + 1, pl.ds(off, p.NZ), :] = part
            G[s + 1, pl.ds(off, p.NZ), :] = part * C[s]
        wrap(W)
        wrap(G)
        accs = [zero] * (j + 2)
        for s in range(p.slabs):
            keep = inside(s)

            def apply(t, carry, s=s, keep=keep, j=j, cur=cur, prev=prev, new=new):
                z = pl.multiple_of(t * SUB, SUB)
                rows = pl.ds(z, SUB)
                w = basis[j, s, rows, :]
                inner = combine(tile_of(G, s, z), ki, None, None, nx)
                outer = combine(tile_of(W, s, z), ke, None, None, nx)
                e = (CS[s, rows, :] + ke_twice) * w - C[s, rows, :] * inner - outer
                e = jnp.where(keep, e, 0.0)
                if j < p.depth - 1:
                    b = cur[s, rows, :]
                    if j == 0:
                        new[s, rows, :] = 0.5 * quarter * e - b
                    else:
                        new[s, rows, :] = quarter * e - 2.0 * b - prev[s, rows, :]
                res = [carry[i] + basis[i, s, rows, :] * e for i in range(j)]
                res.append(carry[j] + w * e)
                res.append(carry[j + 1] + w * recv_b0(s, t))
                return tuple(res)

            def recv_b0(s, t):
                per = p.nz // SUB
                return recv[t // per, pl.ds(pl.multiple_of(s * p.nz + (t % per) * SUB, SUB), SUB), :]

            got = lax.fori_loop(0, zts, apply, tuple([zero] * (j + 2)))
            mine = own(s)
            accs = [a + jnp.where(mine, g, 0.0) for a, g in zip(accs, got)]
        out = lane_put(out, accs[j + 1], j)
        for i in range(j + 1):
            out = lane_put(out, accs[i], slot)
            slot += 1
    sums[...] = jnp.broadcast_to(out, sums.shape)


def solve_kernel(plan, recv, basis, send):
    p = plan
    nx, n = p.nx, p.depth
    tot = jnp.sum(recv[...], axis=0, keepdims=True)

    def get(k):
        return jnp.broadcast_to(tot[:, k : k + 1], (SUB, nx))

    rhs = [get(j) for j in range(n)]
    A = [[None] * n for _ in range(n)]
    slot = n
    for j in range(n):
        for i in range(j + 1):
            A[i][j] = A[j][i] = get(slot)
            slot += 1
    diag = [A[i][i] for i in range(n)]
    inv = [None] * n
    for k in range(n):
        ok = A[k][k] > 1e-7 * diag[k]
        inv[k] = jnp.where(ok, 1.0 / jnp.where(ok, A[k][k], 1.0), 0.0)
        for i in range(k + 1, n):
            m = A[i][k] * inv[k]
            for l in range(k + 1, n):
                A[i][l] = A[i][l] - m * A[k][l]
            rhs[i] = rhs[i] - m * rhs[k]
    sol = [None] * n
    for k in reversed(range(n)):
        acc = rhs[k]
        for l in range(k + 1, n):
            acc = acc - A[k][l] * sol[l]
        sol[k] = acc * inv[k]

    lane = lax.broadcasted_iota(jnp.int32, (SUB, nx), 1)
    group = lane // p.cols
    per = p.nz // SUB

    def pack(t, carry):
        rows = pl.ds(pl.multiple_of(t * SUB, SUB), SUB)
        dst = t // per
        part = []
        for s in range(p.slabs):
            acc = sol[0] * basis[0, s, rows, :]
            for i in range(1, n):
                acc = acc + sol[i] * basis[i, s, rows, :]
            part.append(acc)
        for o in range(p.back):
            acc = None
            for q2 in range(p.back_grp):
                y = p.depth + o * p.back_grp + q2
                q, s = y // p.slabs, y % p.slabs
                amount = (p.cols * q2 - (p.wid * q + p.hx)) % nx
                piece = pltpu.roll(part[s], amount, 1) if amount else part[s]
                acc = piece if acc is None else jnp.where(group == q2, piece, acc)
            send[dst, pl.ds(pl.multiple_of(o * p.nz + (t % per) * SUB, SUB), SUB), :] = acc
        return carry

    lax.fori_loop(0, p.NZ // SUB, pack, 0)


def finish_kernel(plan, recv, pot, out):
    p = plan
    nx = p.nx
    lane = lax.broadcasted_iota(jnp.int32, (SUB, nx), 1)
    group = lane // p.cols
    fpot = pot.reshape(p.nz * p.ny, nx)
    fout = out.reshape(p.nz * p.ny, nx)
    for o in range(p.back):
        for zt in range(p.nz // SUB):
            src = [recv[j, pl.ds(o * p.nz + zt * SUB, SUB), :] for j in range(p.ngx)]
            for q2 in range(p.back_grp):
                acc = None
                for j in range(p.ngx):
                    amount = (p.cols * j - p.cols * q2) % nx
                    piece = pltpu.roll(src[j], amount, 1) if amount else src[j]
                    acc = piece if acc is None else jnp.where(group == j, piece, acc)
                rows = pl.ds(zt * SUB * p.ny + o * p.back_grp + q2, SUB, stride=p.ny)
                fout[rows, :] = fpot[rows, :] + acc


def body(voltage, potential, tissue, gain, couplings, line_factor):
    ngx, ngy = lax.axis_size("gx"), lax.axis_size("gy")
    p = Plan(voltage.shape, ngx, ngy)
    nz, ny, nx = p.nz, p.ny, p.nx
    idx = jnp.stack([lax.axis_index("gx"), lax.axis_index("gy")]).astype(jnp.int32)
    sds = jax.ShapeDtypeStruct

    def call(kernel, name, ins, outs, scratch=()):
        return pl.pallas_call(
            kernel,
            name=name,
            out_shape=outs,
            in_specs=ins,
            out_specs=[VMEM] * len(outs),
            scratch_shapes=list(scratch),
            compiler_params=pltpu.CompilerParams(vmem_limit_bytes=60000 * 1024),
        )

    ysends = [None] if p.swap else [1, -1]
    shapes, routes = [], []

    def pairs(dz, dy):
        res = []
        for a in range(ngx):
            for b in range(ngy):
                if dy is None:
                    tb = (b + 1) % 2
                else:
                    tb = b + dy
                if 0 <= a + dz < ngx and 0 <= tb < ngy:
                    res.append((a * ngy + b, (a + dz) * ngy + tb))
        return res

    for dy in ysends:
        shapes.append(sds((3, nz, p.hy, nx), f32))
        routes.append((0, dy))
    for hop, n in p.hops:
        for sign in (1, -1):
            shapes.append(sds((3, n, ny, nx), f32))
            routes.append((sign * hop, 0))
            for dy in ysends:
                shapes.append(sds((3, n, p.hy, nx), f32))
                routes.append((sign * hop, dy))

    cond, *pieces = call(
        lambda *a: prep_kernel(p, *a), "prep", [SMEM] + [VMEM] * 4, [sds(voltage.shape, f32)] + shapes
    )(idx, voltage, potential, tissue, gain)
    halos = [lax.ppermute(x, ("gx", "gy"), pairs(*r)) for x, r in zip(pieces, routes)]

    n_line = line_factor.shape[0]
    hi, lo, size = call(
        factor_kernel,
        "factor",
        [VMEM] * 2,
        [sds((n_line, n_line), jnp.bfloat16), sds((n_line, n_line), jnp.bfloat16), sds((SUB, nx), f32)],
    )(line_factor, line_factor.T)

    ext = pltpu.VMEM((p.yrows, p.zrows, nx), f32)
    new_voltage, send = call(
        lambda *a: cheb_kernel(p, *a),
        "cheb",
        [SMEM, SMEM] + [VMEM] * (3 + len(halos)),
        [sds(voltage.shape, f32), sds((ngx, 2 * p.slabs * nz, nx), f32)],
        [ext] * 8,
    )(idx, couplings, voltage, potential, cond, *halos)

    recv = lax.all_to_all(send, "gx", split_axis=0, concat_axis=0, tiled=True)

    line = pltpu.VMEM((p.slabs, p.NZ, nx), f32)
    wide = pltpu.VMEM((p.slabs + 2, p.NZ + 2 * SUB, nx), f32)
    half = pltpu.VMEM((p.NZ, p.slabs * nx), jnp.bfloat16)
    basis, sums = call(
        lambda *a: basis_kernel(p, *a),
        "basis",
        [SMEM, SMEM] + [VMEM] * 4,
        [sds((p.depth, p.slabs, p.NZ, nx), f32), sds((ngx * ngy, nx), f32)],
        [line, line, wide, wide, line, line, line, half, half],
    )(idx, couplings, recv, hi, lo, size)

    parts = lax.all_to_all(
        sums.reshape(ngx * ngy, 1, nx), ("gx", "gy"), split_axis=0, concat_axis=0, tiled=True
    ).reshape(ngx * ngy, nx)

    (back,) = call(
        lambda *a: solve_kernel(p, *a), "solve", [VMEM] * 2, [sds((ngx, p.back * nz, nx), f32)]
    )(parts, basis)
    home = lax.all_to_all(back, "gx", split_axis=0, concat_axis=0, tiled=True)
    (new_potential,) = call(
        lambda *a: finish_kernel(p, *a), "finish", [VMEM] * 2, [sds(voltage.shape, f32)]
    )(home, potential)
    return new_voltage, new_potential


def solution(mesh):
    spec = P("gx", "gy", None)
    return jax.shard_map(
        body,
        mesh=mesh,
        in_specs=(spec, spec, spec, spec, P(), P()),
        out_specs=(spec, spec),
        check_vma=False,
    )
```

```python
import jax
import jax.numpy as jnp
from jax import lax
from jax.experimental import pallas as pl
from jax.experimental.pallas import tpu as pltpu
from jax.sharding import PartitionSpec as P

CHEB = 8
ITERS = 4
SUB = 8
ROWS = 4
TILES = 8

time_step = 2.0
ionic_rate = 0.5
onset_level = 0.2
gain_top = 3.0625
f32 = jnp.float32
VMEM = pl.BlockSpec(memory_space=pltpu.VMEM)
SMEM = pl.BlockSpec(memory_space=pltpu.SMEM)


def up_to(n, m):
    return -(-n // m) * m


class Plan:
    def __init__(self, local_shape, ngx, ngy):
        self.nz, self.ny, self.nx = local_shape
        self.ngx, self.ngy = ngx, ngy
        self.depth = ITERS
        self.hz = CHEB + 1
        self.hy = up_to(CHEB + 1 + ITERS, SUB)
        self.swap = ngy == 2
        self.hops = []
        left, hop = self.hz, 1
        while left > 0:
            self.hops.append((hop, min(self.nz, left)))
            left -= self.nz
            hop += 1
        self.pad = up_to(ITERS + 1, SUB)
        self.ywin = self.ny + self.hy * (1 if self.swap else 2)
        self.yrows = self.ywin + 2 * self.pad
        self.zrows = up_to(max(self.hz - d + up_to(self.nz + 2 * d, SUB) + 1 for d in range(self.hz)), SUB)
        self.zrows = max(self.zrows, up_to(self.nz + 2 * self.hz, SUB))
        self.NZ = self.nz * ngx
        self.cols = self.nx // ngx
        self.wid = 1
        while self.wid < self.cols + 2 * self.depth:
            self.wid *= 2
        self.hx = (self.wid - self.cols) // 2
        self.grp = self.nx // self.wid
        self.slabs = -(-(self.ny + 2 * self.depth) // self.grp)
        self.back_grp = self.nx // self.cols
        self.back = self.ny // self.back_grp


def prep_kernel(plan, idx, volt, pot, tissue, gain, cond, *outs):
    cond[...] = tissue[...].astype(f32) * gain[...]
    fields = (volt, pot, cond)
    if plan.swap:
        ys = [pl.multiple_of((1 - idx[1]) * (plan.ny - plan.hy), SUB)]
    else:
        ys = [plan.ny - plan.hy, 0]
    at = 0
    for y0 in ys:
        for f, ref in enumerate(fields):
            outs[at][f] = ref[:, pl.ds(y0, plan.hy), :]
        at += 1
    for _, n in plan.hops:
        for z0 in (plan.nz - n, 0):
            for f, ref in enumerate(fields):
                outs[at][f] = ref[pl.ds(z0, n)]
            at += 1
            for y0 in ys:
                for f, ref in enumerate(fields):
                    outs[at][f] = ref[pl.ds(z0, n), pl.ds(y0, plan.hy), :]
                at += 1


def combine(tile, coef, left, right, width):
    k = coef
    mid, zp, zm, yp, ym = tile(0, 0), tile(1, 0), tile(-1, 0), tile(0, 1), tile(0, -1)
    zpyp, zmym, zpym, zmyp = tile(1, 1), tile(-1, -1), tile(1, -1), tile(-1, 1)
    same = k[0] * (zp + zm) + k[1] * (yp + ym) + k[3] * (zpyp + zmym) + k[4] * (zpym + zmyp)
    face = k[2] * mid
    plus = face + k[5] * zp + k[6] * zm + k[7] * yp + k[8] * ym
    minus = face + k[5] * zm + k[6] * zp + k[7] * ym + k[8] * yp
    plus = pltpu.roll(plus, width - 1, 1)
    minus = pltpu.roll(minus, 1, 1)
    if left is not None:
        plus = jnp.where(right, 0.0, plus)
        minus = jnp.where(left, 0.0, minus)
    return same + plus + minus


def cheb_kernel(plan, idx, coup, volt, pot, cond, *rest):
    p = plan
    ny_halo = 1 if p.swap else 2
    n_in = ny_halo + len(p.hops) * 2 * (1 + ny_halo)
    halos = rest[:n_in]
    new_volt, send = rest[n_in : n_in + 2]
    C, G0, G1, E, PT, R, U, CS = rest[n_in + 2 :]
    nx = p.nx
    flat = lambda ref: ref.reshape(p.yrows * p.zrows, nx)
    if p.swap:
        ylocal = p.pad + idx[1] * p.hy
        yhalo = [p.pad + (1 - idx[1]) * p.ny]
    else:
        ylocal = p.pad + p.hy
        yhalo = [p.pad, p.pad + p.hy + p.ny]

    zero_rows = jnp.zeros((p.pad, p.zrows, nx), f32)
    for ref in (C, G0, G1, E, PT, R, U, CS):
        ref[pl.ds(0, p.pad)] = zero_rows
        ref[pl.ds(p.pad + p.ywin, p.pad)] = zero_rows

    fc, fg, fe, fp, fr = (flat(r) for r in (C, G0, E, PT, R))

    def place(getter, planes, zrow0, yrow0, ycount):
        def one(z, carry):
            for t in range(ycount // SUB):
                v, q, c = getter(z, t)
                start = (yrow0 + t * SUB) * p.zrows + zrow0 + z
                rows = pl.ds(start, SUB, stride=p.zrows)
                s = v + q
                mask = jnp.where(c > 0.0, 1.0, 0.0)
                fc[rows, :] = c
                fg[rows, :] = c * s
                fe[rows, :] = s
                fp[rows, :] = q
                fr[rows, :] = (-ionic_rate) * mask * v * (v - onset_level) * (v - 1.0)
            return carry

        lax.fori_loop(0, planes, one, 0)

    def local(z, t):
        ys = pl.ds(t * SUB, SUB)
        return volt[z, ys, :], pot[z, ys, :], cond[z, ys, :]

    def piece(ref):
        def get(z, t):
            ys = pl.ds(t * SUB, SUB)
            return ref[0, z, ys, :], ref[1, z, ys, :], ref[2, z, ys, :]

        return get

    place(local, p.nz, p.hz, ylocal, p.ny)
    at = 0
    for y0 in yhalo:
        place(piece(halos[at]), p.nz, p.hz, y0, p.hy)
        at += 1
    done = 0
    for _, n in p.hops:
        for z0 in (p.hz - done - n, p.hz + p.nz + done):
            place(piece(halos[at]), n, z0, ylocal, p.ny)
            at += 1
            for y0 in yhalo:
                place(piece(halos[at]), n, z0, y0, p.hy)
                at += 1
        done += n

    lane = lax.broadcasted_iota(jnp.int32, (SUB, nx), 1)
    left, right = lane == 0, lane == nx - 1
    ki = [coup[0, k] for k in range(9)]
    ke = [coup[1, k] for k in range(9)]

    total = ki[0]
    for k in ki[1:]:
        total = total + k
    top = 1.0 + time_step * 4.0 * gain_top * jnp.full((SUB, nx), total, f32)
    centre = (top + 1.0) / 2.0
    half = (top - 1.0) / 2.0
    ratio = centre / half
    weight = 1.0 / ratio
    inv_centre = 1.0 / centre

    def sweep(d, body):
        tiles = up_to(p.nz + 2 * d, SUB) // SUB
        over = p.hy - p.depth - d
        y0 = p.pad + (idx[1] * over if p.swap else over)
        count = p.ny + (d + p.depth) * (1 if p.swap else 2)

        def block(i, carry):
            stores = []
            for r in range(ROWS):
                for t in range(tiles):
                    stores += body(y0 + i * ROWS + r, p.hz - d + t * SUB)
            for ref, where, value in stores:
                ref[where] = value
            return carry

        lax.fori_loop(0, -(-count // ROWS), block, 0)

    def tile_of(ref, y, z):
        return lambda dz, dy: ref[y + dy, pl.ds(z + dz, SUB), :]

    def first(y, z):
        rows = pl.ds(z, SUB)
        c = C[y, rows, :]
        s = E[y, rows, :]
        cs = c * combine(tile_of(C, y, z), ki, left, right, nx)
        flow = cs * s - c * combine(tile_of(G0, y, z), ki, left, right, nx)
        r = R[y, rows, :] - time_step * flow
        u = r * inv_centre
        at = (y, rows)
        return [(CS, at, cs), (R, at, r), (U, at, u), (E, at, s + u), (G1, at, c * u)]

    sweep(CHEB, first)
    bufs = [G0, G1]
    for k in range(1, CHEB):
        gin, gout = bufs[k % 2], bufs[(k + 1) % 2]
        nxt = 1.0 / (2.0 * ratio - weight)
        keep, add = nxt * weight, 2.0 * nxt / half
        weight = nxt
        last = k == CHEB - 1

        def step(y, z, gin=gin, gout=gout, keep=keep, add=add, last=last):
            rows = pl.ds(z, SUB)
            c = C[y, rows, :]
            u = U[y, rows, :]
            flow = CS[y, rows, :] * u - c * combine(tile_of(gin, y, z), ki, left, right, nx)
            r = R[y, rows, :] - (u + time_step * flow)
            u = keep * u + add * r
            e = E[y, rows, :] + u
            at = (y, rows)
            if last:
                return [(E, at, e), (gout, at, c * e)]
            return [(E, at, e), (R, at, r), (U, at, u), (gout, at, c * u)]

        sweep(CHEB - k, step)

    gin = bufs[CHEB % 2]
    ke_sum = ke[0]
    for k in ke[1:]:
        ke_sum = ke_sum + k
    ke_sum = 2.0 * ke_sum

    def final(y, z):
        rows = pl.ds(z, SUB)
        c = C[y, rows, :]
        flow = CS[y, rows, :] * E[y, rows, :] - c * combine(tile_of(gin, y, z), ki, left, right, nx)
        outer = ke_sum * PT[y, rows, :] - combine(tile_of(PT, y, z), ke, left, right, nx)
        return [(R, (y, rows), -flow - outer)]

    sweep(0, final)

    def give(z, carry):
        for t in range(p.ny // SUB):
            start = (ylocal + t * SUB) * p.zrows + p.hz + z
            rows = pl.ds(start, SUB, stride=p.zrows)
            new_volt[z, pl.ds(t * SUB, SUB), :] = fe[rows, :] - fp[rows, :]
        return carry

    lax.fori_loop(0, p.nz, give, 0)

    group = lane // p.wid
    first_row = ylocal - p.depth

    def pack(s, carry):
        for f, ref in enumerate((R, C)):
            for zt in range(p.nz // SUB):
                src = [ref[first_row + q * p.slabs + s, pl.ds(p.hz + zt * SUB, SUB), :] for q in range(p.grp)]
                for j in range(p.ngx):
                    acc = None
                    for q in range(p.grp):
                        amount = (p.wid * q - (p.cols * j - p.hx)) % nx
                        part = pltpu.roll(src[q], amount, 1) if amount else src[q]
                        acc = part if acc is None else jnp.where(group == q, part, acc)
                    row = (f * p.slabs + s) * p.nz + zt * SUB
                    send[j, pl.ds(pl.multiple_of(row, SUB), SUB), :] = acc
        return carry

    lax.fori_loop(0, p.slabs, pack, 0)


def factor_kernel(line, line_t, parts, size):
    scale = 1.0 / jnp.max(jnp.abs(line[...]), keepdims=True)
    a = line_t[...] * scale
    b = line[...] * scale
    g = jnp.dot(a, b, precision=lax.Precision.HIGHEST, preferred_element_type=f32)
    high = g.astype(jnp.bfloat16)
    n = g.shape[0]
    parts[:, pl.ds(0, n)] = high
    parts[:, pl.ds(n, n)] = (g - high.astype(f32)).astype(jnp.bfloat16)
    parts[:, pl.ds(2 * n, n)] = high

    def norm(m):
        return jnp.sqrt(jnp.sum(jnp.sum(m * m, axis=0, keepdims=True), axis=1, keepdims=True))

    n = norm(g)
    est = n
    m = g / n
    for power in range(3):
        mb = m.astype(jnp.bfloat16)
        m = jnp.dot(mb, mb, preferred_element_type=f32)
        n = norm(m)
        m = m / n
        root = n
        for _ in range(power + 1):
            root = jnp.sqrt(root)
        est = est * root
    size[...] = jnp.broadcast_to(est, size.shape)


def basis_kernel(plan, idx, coup, recv, factor, size, basis, sums, C, CS, G, W, B0, B1, B2, R0, BB):
    p = plan
    nx, off = p.nx, SUB
    lane = lax.broadcasted_iota(jnp.int32, (SUB, nx), 1)
    x = p.cols * idx[0] - p.hx + lane % p.wid
    xin = (x >= 0) & (x < nx)
    xown = (lane % p.wid >= p.hx) & (lane % p.wid < p.hx + p.cols)
    ki = [coup[0, k] for k in range(9)]
    ke = [coup[1, k] for k in range(9)]
    ki_sum, ke_sum = ki[0], ke[0]
    for k in range(1, 9):
        ki_sum = ki_sum + ki[k]
        ke_sum = ke_sum + ke[k]
    lam = 2.0 * (ki_sum + ke_sum) * size[...]
    quarter = 4.0 / lam
    ke_twice = 2.0 * ke_sum

    def ywin(s):
        return (lane // p.wid) * p.slabs + s

    def inside(s):
        y = p.ny * idx[1] - p.depth + ywin(s)
        return xin & (y >= 0) & (y < p.ny * p.ngy)

    def own(s):
        return xown & (ywin(s) >= p.depth) & (ywin(s) < p.depth + p.ny)

    for ref in (G, W):
        for s in range(p.slabs + 2):
            ref[s, pl.ds(0, off), :] = jnp.zeros((off, nx), f32)
            ref[s, pl.ds(off + p.NZ, off), :] = jnp.zeros((off, nx), f32)

    for s in range(p.slabs):
        keep = inside(s)
        for j in range(p.ngx):
            for zt in range(p.nz // SUB):
                rows = pl.ds(j * p.nz + zt * SUB, SUB)
                b = jnp.where(keep, recv[j, pl.ds(s * p.nz + zt * SUB, SUB), :], 0.0)
                B0[s, rows, :] = b
                R0[s, rows, :] = b
                c = jnp.where(keep, recv[j, pl.ds((p.slabs + s) * p.nz + zt * SUB, SUB), :], 0.0)
                C[s, rows, :] = c
                G[s + 1, pl.ds(off + j * p.nz + zt * SUB, SUB), :] = c

    def wrap(ref):
        body = pl.ds(off, p.NZ)
        ref[0, body, :] = pltpu.roll(ref[p.slabs, body, :], p.wid, 1)
        ref[p.slabs + 1, body, :] = pltpu.roll(ref[1, body, :], nx - p.wid, 1)

    wrap(G)

    def tile_of(ref, s, z):
        return lambda dz, dy: ref[s + 1 + dy, pl.ds(off + z + dz, SUB), :]

    step = TILES * SUB
    for s in range(p.slabs):

        def weigh(t, carry, s=s):
            vals = []
            for k in range(TILES):
                z = pl.multiple_of(t * step, step) + k * SUB
                vals.append((z, C[s, pl.ds(z, SUB), :] * combine(tile_of(G, s, z), ki, None, None, nx)))
            for z, v in vals:
                CS[s, pl.ds(z, SUB), :] = v
            return carry

        lax.fori_loop(0, p.NZ // step, weigh, 0)

    ring = [B0, B1, B2]
    out = jnp.zeros((1, nx), f32)

    def lane_put(out, acc, at):
        v = jnp.sum(jnp.sum(acc, axis=1, keepdims=True), axis=0, keepdims=True)
        return jnp.where(lax.broadcasted_iota(jnp.int32, (1, nx), 1) == at, v, out)

    zero = jnp.zeros((SUB, nx), f32)
    slot = p.depth
    for j in range(p.depth):
        cur = ring[j % 3]
        prev = ring[(j + 2) % 3]
        new = ring[(j + 1) % 3]
        for s in range(p.slabs):
            b = cur[s]
            high = b.astype(jnp.bfloat16)
            cols = pl.ds(s * nx, nx)
            BB[pl.ds(0, p.NZ), cols] = high
            BB[pl.ds(p.NZ, p.NZ), cols] = high
            BB[pl.ds(2 * p.NZ, p.NZ), cols] = (b - high.astype(f32)).astype(jnp.bfloat16)
        prod = jnp.dot(factor[...], BB[...], preferred_element_type=f32)
        for s in range(p.slabs):
            part = prod[:, s * nx : (s + 1) * nx]
            basis[j, s] = part
            W[s + 1, pl.ds(off, p.NZ), :] = part
            G[s + 1, pl.ds(off, p.NZ), :] = part * C[s]
        wrap(W)
        wrap(G)
        accs = [zero] * (j + 2)
        for s in range(p.slabs):
            keep = inside(s)

            def apply(t, carry, s=s, keep=keep, j=j, cur=cur, prev=prev, new=new):
                res = list(carry)
                stores = []
                for k in range(TILES):
                    z = pl.multiple_of(t * step, step) + k * SUB
                    rows = pl.ds(z, SUB)
                    w = W[s + 1, pl.ds(off + z, SUB), :]
                    inner = combine(tile_of(G, s, z), ki, None, None, nx)
                    outer = combine(tile_of(W, s, z), ke, None, None, nx)
                    e = (CS[s, rows, :] + ke_twice) * w - C[s, rows, :] * inner - outer
                    e = jnp.where(keep, e, 0.0)
                    if j < p.depth - 1:
                        b = cur[s, rows, :]
                        if j == 0:
                            stores.append((rows, 0.5 * quarter * e - b))
                        else:
                            stores.append((rows, quarter * e - 2.0 * b - prev[s, rows, :]))
                    for i in range(j):
                        res[i] = res[i] + basis[i, s, rows, :] * e
                    res[j] = res[j] + w * e
                    res[j + 1] = res[j + 1] + w * R0[s, rows, :]
                for rows, value in stores:
                    new[s, rows, :] = value
                return tuple(res)

            got = lax.fori_loop(0, p.NZ // step, apply, tuple([zero] * (j + 2)))
            mine = own(s)
            accs = [a + jnp.where(mine, g, 0.0) for a, g in zip(accs, got)]
        out = lane_put(out, accs[j + 1], j)
        for i in range(j + 1):
            out = lane_put(out, accs[i], slot)
            slot += 1
    sums[...] = jnp.broadcast_to(out, sums.shape)


def solve_kernel(plan, recv, basis, send):
    p = plan
    nx, n = p.nx, p.depth
    tot = jnp.sum(recv[...], axis=0, keepdims=True)

    def get(k):
        return jnp.broadcast_to(tot[:, k : k + 1], (SUB, nx))

    rhs = [get(j) for j in range(n)]
    A = [[None] * n for _ in range(n)]
    slot = n
    for j in range(n):
        for i in range(j + 1):
            A[i][j] = A[j][i] = get(slot)
            slot += 1
    diag = [A[i][i] for i in range(n)]
    inv = [None] * n
    for k in range(n):
        ok = A[k][k] > 1e-7 * diag[k]
        inv[k] = jnp.where(ok, 1.0 / jnp.where(ok, A[k][k], 1.0), 0.0)
        for i in range(k + 1, n):
            m = A[i][k] * inv[k]
            for l in range(k + 1, n):
                A[i][l] = A[i][l] - m * A[k][l]
            rhs[i] = rhs[i] - m * rhs[k]
    sol = [None] * n
    for k in reversed(range(n)):
        acc = rhs[k]
        for l in range(k + 1, n):
            acc = acc - A[k][l] * sol[l]
        sol[k] = acc * inv[k]

    lane = lax.broadcasted_iota(jnp.int32, (SUB, nx), 1)
    group = lane // p.cols
    per = p.nz // SUB

    def pack(t, carry):
        rows = pl.ds(pl.multiple_of(t * SUB, SUB), SUB)
        dst = t // per
        part = []
        for s in range(p.slabs):
            acc = sol[0] * basis[0, s, rows, :]
            for i in range(1, n):
                acc = acc + sol[i] * basis[i, s, rows, :]
            part.append(acc)
        for o in range(p.back):
            acc = None
            for q2 in range(p.back_grp):
                y = p.depth + o * p.back_grp + q2
                q, s = y // p.slabs, y % p.slabs
                amount = (p.cols * q2 - (p.wid * q + p.hx)) % nx
                piece = pltpu.roll(part[s], amount, 1) if amount else part[s]
                acc = piece if acc is None else jnp.where(group == q2, piece, acc)
            send[dst, pl.ds(pl.multiple_of(o * p.nz + (t % per) * SUB, SUB), SUB), :] = acc
        return carry

    lax.fori_loop(0, p.NZ // SUB, pack, 0, unroll=2)


def finish_kernel(plan, recv, pot, out):
    p = plan
    nx = p.nx
    lane = lax.broadcasted_iota(jnp.int32, (SUB, nx), 1)
    group = lane // p.cols
    fpot = pot.reshape(p.nz * p.ny, nx)
    fout = out.reshape(p.nz * p.ny, nx)
    for o in range(p.back):
        for zt in range(p.nz // SUB):
            src = [recv[j, pl.ds(o * p.nz + zt * SUB, SUB), :] for j in range(p.ngx)]
            for q2 in range(p.back_grp):
                acc = None
                for j in range(p.ngx):
                    amount = (p.cols * j - p.cols * q2) % nx
                    piece = pltpu.roll(src[j], amount, 1) if amount else src[j]
                    acc = piece if acc is None else jnp.where(group == j, piece, acc)
                rows = pl.ds(zt * SUB * p.ny + o * p.back_grp + q2, SUB, stride=p.ny)
                fout[rows, :] = fpot[rows, :] + acc


def body(voltage, potential, tissue, gain, couplings, line_factor):
    ngx, ngy = lax.axis_size("gx"), lax.axis_size("gy")
    p = Plan(voltage.shape, ngx, ngy)
    nz, ny, nx = p.nz, p.ny, p.nx
    idx = jnp.stack([lax.axis_index("gx"), lax.axis_index("gy")]).astype(jnp.int32)
    sds = jax.ShapeDtypeStruct

    def call(kernel, name, ins, outs, scratch=()):
        return pl.pallas_call(
            kernel,
            name=name,
            out_shape=outs,
            in_specs=ins,
            out_specs=[VMEM] * len(outs),
            scratch_shapes=list(scratch),
            compiler_params=pltpu.CompilerParams(vmem_limit_bytes=60000 * 1024),
        )

    ysends = [None] if p.swap else [1, -1]
    shapes, routes = [], []

    def pairs(dz, dy):
        res = []
        for a in range(ngx):
            for b in range(ngy):
                if dy is None:
                    tb = (b + 1) % 2
                else:
                    tb = b + dy
                if 0 <= a + dz < ngx and 0 <= tb < ngy:
                    res.append((a * ngy + b, (a + dz) * ngy + tb))
        return res

    for dy in ysends:
        shapes.append(sds((3, nz, p.hy, nx), f32))
        routes.append((0, dy))
    for hop, n in p.hops:
        for sign in (1, -1):
            shapes.append(sds((3, n, ny, nx), f32))
            routes.append((sign * hop, 0))
            for dy in ysends:
                shapes.append(sds((3, n, p.hy, nx), f32))
                routes.append((sign * hop, dy))

    cond, *pieces = call(
        lambda *a: prep_kernel(p, *a), "prep", [SMEM] + [VMEM] * 4, [sds(voltage.shape, f32)] + shapes
    )(idx, voltage, potential, tissue, gain)
    halos = [lax.ppermute(x, ("gx", "gy"), pairs(*r)) for x, r in zip(pieces, routes)]

    n_line = line_factor.shape[0]
    parts, size = call(
        factor_kernel,
        "factor",
        [VMEM] * 2,
        [sds((n_line, 3 * n_line), jnp.bfloat16), sds((SUB, nx), f32)],
    )(line_factor, line_factor.T)

    ext = pltpu.VMEM((p.yrows, p.zrows, nx), f32)
    new_voltage, send = call(
        lambda *a: cheb_kernel(p, *a),
        "cheb",
        [SMEM, SMEM] + [VMEM] * (3 + len(halos)),
        [sds(voltage.shape, f32), sds((ngx, 2 * p.slabs * nz, nx), f32)],
        [ext] * 8,
    )(idx, couplings, voltage, potential, cond, *halos)

    recv = lax.all_to_all(send, "gx", split_axis=0, concat_axis=0, tiled=True)

    line = pltpu.VMEM((p.slabs, p.NZ, nx), f32)
    wide = pltpu.VMEM((p.slabs + 2, p.NZ + 2 * SUB, nx), f32)
    half = pltpu.VMEM((3 * p.NZ, p.slabs * nx), jnp.bfloat16)
    basis, sums = call(
        lambda *a: basis_kernel(p, *a),
        "basis",
        [SMEM, SMEM] + [VMEM] * 3,
        [sds((p.depth, p.slabs, p.NZ, nx), f32), sds((ngx * ngy, nx), f32)],
        [line, line, wide, wide, line, line, line, line, half],
    )(idx, couplings, recv, parts, size)

    shares = lax.all_to_all(
        sums.reshape(ngx * ngy, 1, nx), ("gx", "gy"), split_axis=0, concat_axis=0, tiled=True
    ).reshape(ngx * ngy, nx)

    (back,) = call(
        lambda *a: solve_kernel(p, *a), "solve", [VMEM] * 2, [sds((ngx, p.back * nz, nx), f32)]
    )(shares, basis)
    home = lax.all_to_all(back, "gx", split_axis=0, concat_axis=0, tiled=True)
    (new_potential,) = call(
        lambda *a: finish_kernel(p, *a), "finish", [VMEM] * 2, [sds(voltage.shape, f32)]
    )(home, potential)
    return new_voltage, new_potential


def solution(mesh):
    spec = P("gx", "gy", None)
    return jax.shard_map(
        body,
        mesh=mesh,
        in_specs=(spec, spec, spec, spec, P(), P()),
        out_specs=(spec, spec),
        check_vma=False,
    )
```

```python
import jax
import jax.numpy as jnp
from jax import lax
from jax.experimental import pallas as pl
from jax.experimental.pallas import tpu as pltpu
from jax.sharding import PartitionSpec as P


CHEB = 8
ITERS = 4
SUB = 8
ROWS = 4
TILES = 8

time_step = 2.0
ionic_rate = 0.5
onset_level = 0.2
gain_top = 3.0625
f32 = jnp.float32
VMEM = pl.BlockSpec(memory_space=pltpu.VMEM)
SMEM = pl.BlockSpec(memory_space=pltpu.SMEM)


def up_to(n, m):
    return -(-n // m) * m


class Plan:
    def __init__(self, local_shape, ngx, ngy):
        self.nz, self.ny, self.nx = local_shape
        self.ngx, self.ngy = ngx, ngy
        self.depth = ITERS
        self.hz = CHEB + 1
        self.hy = up_to(CHEB + 1 + ITERS, SUB)
        self.swap = ngy == 2
        self.hops = []
        left, hop = self.hz, 1
        while left > 0:
            self.hops.append((hop, min(self.nz, left)))
            left -= self.nz
            hop += 1
        self.pad = up_to(ITERS + 1, SUB)
        self.ywin = self.ny + self.hy * (1 if self.swap else 2)
        self.yrows = self.ywin + 2 * self.pad
        self.zrows = up_to(max(self.hz - d + up_to(self.nz + 2 * d, SUB) + 1 for d in range(self.hz)), SUB)
        self.zrows = max(self.zrows, up_to(self.nz + 2 * self.hz, SUB))
        self.NZ = self.nz * ngx
        self.cols = self.nx // ngx
        self.wid = 1
        while self.wid < self.cols + 2 * self.depth:
            self.wid *= 2
        self.hx = (self.wid - self.cols) // 2
        self.grp = self.nx // self.wid
        self.slabs = -(-(self.ny + 2 * self.depth) // self.grp)
        self.back_grp = self.nx // self.cols
        self.back = self.ny // self.back_grp


def here():
    return lax.axis_index("gx"), lax.axis_index("gy")


def prep_kernel(plan, volt, pot, tissue, gain, cond, *outs):
    idx = here()
    cond[...] = tissue[...].astype(f32) * gain[...]
    fields = (volt, pot, cond)
    if plan.swap:
        ys = [pl.multiple_of((1 - idx[1]) * (plan.ny - plan.hy), SUB)]
    else:
        ys = [plan.ny - plan.hy, 0]
    at = 0
    for y0 in ys:
        for f, ref in enumerate(fields):
            outs[at][f] = ref[:, pl.ds(y0, plan.hy), :]
        at += 1
    for _, n in plan.hops:
        for z0 in (plan.nz - n, 0):
            for f, ref in enumerate(fields):
                outs[at][f] = ref[pl.ds(z0, n)]
            at += 1
            for y0 in ys:
                for f, ref in enumerate(fields):
                    outs[at][f] = ref[pl.ds(z0, n), pl.ds(y0, plan.hy), :]
                at += 1


def combine(tile, coef, left, right, width):
    k = coef
    mid, zp, zm, yp, ym = tile(0, 0), tile(1, 0), tile(-1, 0), tile(0, 1), tile(0, -1)
    zpyp, zmym, zpym, zmyp = tile(1, 1), tile(-1, -1), tile(1, -1), tile(-1, 1)
    same = k[0] * (zp + zm) + k[1] * (yp + ym) + k[3] * (zpyp + zmym) + k[4] * (zpym + zmyp)
    face = k[2] * mid
    plus = face + k[5] * zp + k[6] * zm + k[7] * yp + k[8] * ym
    minus = face + k[5] * zm + k[6] * zp + k[7] * ym + k[8] * yp
    plus = pltpu.roll(plus, width - 1, 1)
    minus = pltpu.roll(minus, 1, 1)
    if left is not None:
        plus = jnp.where(right, 0.0, plus)
        minus = jnp.where(left, 0.0, minus)
    return same + plus + minus


def cheb_kernel(plan, coup, volt, pot, cond, *rest):
    p = plan
    idx = here()
    ny_halo = 1 if p.swap else 2
    n_in = ny_halo + len(p.hops) * 2 * (1 + ny_halo)
    halos = rest[:n_in]
    new_volt, send = rest[n_in : n_in + 2]
    C, G0, G1, E, PT, R, U, CS = rest[n_in + 2 :]
    nx = p.nx
    flat = lambda ref: ref.reshape(p.yrows * p.zrows, nx)
    if p.swap:
        ylocal = p.pad + idx[1] * p.hy
        yhalo = [p.pad + (1 - idx[1]) * p.ny]
    else:
        ylocal = p.pad + p.hy
        yhalo = [p.pad, p.pad + p.hy + p.ny]

    zero_rows = jnp.zeros((p.pad, p.zrows, nx), f32)
    for ref in (C, G0, G1, E, PT, R, U, CS):
        ref[pl.ds(0, p.pad)] = zero_rows
        ref[pl.ds(p.pad + p.ywin, p.pad)] = zero_rows

    fc, fg, fe, fp, fr = (flat(r) for r in (C, G0, E, PT, R))

    def place(getter, planes, zrow0, yrow0, ycount):
        def one(z, carry):
            for t in range(ycount // SUB):
                v, q, c = getter(z, t)
                start = (yrow0 + t * SUB) * p.zrows + zrow0 + z
                rows = pl.ds(start, SUB, stride=p.zrows)
                s = v + q
                mask = jnp.where(c > 0.0, 1.0, 0.0)
                fc[rows, :] = c
                fg[rows, :] = c * s
                fe[rows, :] = s
                fp[rows, :] = q
                fr[rows, :] = (-ionic_rate) * mask * v * (v - onset_level) * (v - 1.0)
            return carry

        lax.fori_loop(0, planes, one, 0)

    def local(z, t):
        ys = pl.ds(t * SUB, SUB)
        return volt[z, ys, :], pot[z, ys, :], cond[z, ys, :]

    def piece(ref):
        def get(z, t):
            ys = pl.ds(t * SUB, SUB)
            return ref[0, z, ys, :], ref[1, z, ys, :], ref[2, z, ys, :]

        return get

    place(local, p.nz, p.hz, ylocal, p.ny)
    at = 0
    for y0 in yhalo:
        place(piece(halos[at]), p.nz, p.hz, y0, p.hy)
        at += 1
    done = 0
    for _, n in p.hops:
        for z0 in (p.hz - done - n, p.hz + p.nz + done):
            place(piece(halos[at]), n, z0, ylocal, p.ny)
            at += 1
            for y0 in yhalo:
                place(piece(halos[at]), n, z0, y0, p.hy)
                at += 1
        done += n

    lane = lax.broadcasted_iota(jnp.int32, (SUB, nx), 1)
    left, right = lane == 0, lane == nx - 1
    ki = [coup[0, k] for k in range(9)]
    ke = [coup[1, k] for k in range(9)]

    total = ki[0]
    for k in ki[1:]:
        total = total + k
    top = 1.0 + time_step * 4.0 * gain_top * jnp.full((SUB, nx), total, f32)
    centre = (top + 1.0) / 2.0
    half = (top - 1.0) / 2.0
    ratio = centre / half
    weight = 1.0 / ratio
    inv_centre = 1.0 / centre

    def sweep(d, body):
        tiles = up_to(p.nz + 2 * d, SUB) // SUB
        over = p.hy - p.depth - d
        y0 = p.pad + (idx[1] * over if p.swap else over)
        count = p.ny + (d + p.depth) * (1 if p.swap else 2)

        def block(i, carry):
            stores = []
            for r in range(ROWS):
                for t in range(tiles):
                    stores += body(y0 + i * ROWS + r, p.hz - d + t * SUB)
            for ref, where, value in stores:
                ref[where] = value
            return carry

        lax.fori_loop(0, -(-count // ROWS), block, 0)

    def tile_of(ref, y, z):
        return lambda dz, dy: ref[y + dy, pl.ds(z + dz, SUB), :]

    def first(y, z):
        rows = pl.ds(z, SUB)
        c = C[y, rows, :]
        s = E[y, rows, :]
        cs = c * combine(tile_of(C, y, z), ki, left, right, nx)
        flow = cs * s - c * combine(tile_of(G0, y, z), ki, left, right, nx)
        r = R[y, rows, :] - time_step * flow
        u = r * inv_centre
        at = (y, rows)
        return [(CS, at, cs), (R, at, r), (U, at, u), (E, at, s + u), (G1, at, c * u)]

    sweep(CHEB, first)
    bufs = [G0, G1]
    for k in range(1, CHEB):
        gin, gout = bufs[k % 2], bufs[(k + 1) % 2]
        nxt = 1.0 / (2.0 * ratio - weight)
        keep, add = nxt * weight, 2.0 * nxt / half
        weight = nxt
        last = k == CHEB - 1

        def step(y, z, gin=gin, gout=gout, keep=keep, add=add, last=last):
            rows = pl.ds(z, SUB)
            c = C[y, rows, :]
            u = U[y, rows, :]
            flow = CS[y, rows, :] * u - c * combine(tile_of(gin, y, z), ki, left, right, nx)
            r = R[y, rows, :] - (u + time_step * flow)
            u = keep * u + add * r
            e = E[y, rows, :] + u
            at = (y, rows)
            if last:
                return [(E, at, e), (gout, at, c * e)]
            return [(E, at, e), (R, at, r), (U, at, u), (gout, at, c * u)]

        sweep(CHEB - k, step)

    gin = bufs[CHEB % 2]
    ke_sum = ke[0]
    for k in ke[1:]:
        ke_sum = ke_sum + k
    ke_sum = 2.0 * ke_sum

    def final(y, z):
        rows = pl.ds(z, SUB)
        c = C[y, rows, :]
        flow = CS[y, rows, :] * E[y, rows, :] - c * combine(tile_of(gin, y, z), ki, left, right, nx)
        outer = ke_sum * PT[y, rows, :] - combine(tile_of(PT, y, z), ke, left, right, nx)
        return [(R, (y, rows), -flow - outer)]

    sweep(0, final)

    def give(z, carry):
        for t in range(p.ny // SUB):
            start = (ylocal + t * SUB) * p.zrows + p.hz + z
            rows = pl.ds(start, SUB, stride=p.zrows)
            new_volt[z, pl.ds(t * SUB, SUB), :] = fe[rows, :] - fp[rows, :]
        return carry

    lax.fori_loop(0, p.nz, give, 0)

    first_row = ylocal - p.depth

    def pack(s, carry):
        for zt in range(p.nz // SUB):
            rows = pl.ds(p.hz + zt * SUB, SUB)
            src = [R[first_row + q * p.slabs + s, rows, :] for q in range(p.grp)]
            windows(p, src, send, pl.multiple_of(s * p.nz + zt * SUB, SUB))
        return carry

    lax.fori_loop(0, p.slabs, pack, 0)


def windows(p, src, send, row):
    group = lax.broadcasted_iota(jnp.int32, (SUB, p.nx), 1) // p.wid
    for j in range(p.ngx):
        acc = None
        for q in range(p.grp):
            amount = (p.wid * q - (p.cols * j - p.hx)) % p.nx
            part = pltpu.roll(src[q], amount, 1) if amount else src[q]
            acc = part if acc is None else jnp.where(group == q, part, acc)
        send[j, pl.ds(row, SUB), :] = acc


def cond_kernel(plan, cond, *rest):
    p = plan
    *sides, send = rest
    idx = here()
    flat = cond.reshape(p.nz * p.ny, p.nx)
    flats = [ref.reshape(3 * p.nz * p.hy, p.nx) for ref in sides]

    def row_of(y, zt):
        if 0 <= y < p.ny:
            return flat[pl.ds(zt * SUB * p.ny + y, SUB, stride=p.ny), :]
        low = y < 0
        at = p.hy + y if low else y - p.ny
        if at >= p.hy:
            return jnp.zeros((SUB, p.nx), f32)
        ref = flats[0] if low else flats[-1]
        val = ref[pl.ds((2 * p.nz + zt * SUB) * p.hy + at, SUB, stride=p.hy), :]
        if p.swap:
            val = jnp.where(idx[1] == (1 if low else 0), val, 0.0)
        return val

    for s in range(p.slabs):
        for zt in range(p.nz // SUB):
            src = [row_of(q * p.slabs + s - p.depth, zt) for q in range(p.grp)]
            windows(p, src, send, s * p.nz + zt * SUB)


def factor_kernel(line, line_t, parts, size):
    scale = 1.0 / jnp.max(jnp.abs(line[...]), keepdims=True)
    a = line_t[...] * scale
    b = line[...] * scale
    g = jnp.dot(a, b, precision=lax.Precision.HIGHEST, preferred_element_type=f32)
    high = g.astype(jnp.bfloat16)
    n = g.shape[0]
    parts[:, pl.ds(0, n)] = high
    parts[:, pl.ds(n, n)] = (g - high.astype(f32)).astype(jnp.bfloat16)
    parts[:, pl.ds(2 * n, n)] = high

    def norm(m):
        return jnp.sqrt(jnp.sum(jnp.sum(m * m, axis=0, keepdims=True), axis=1, keepdims=True))

    n = norm(g)
    est = n
    m = g / n
    for power in range(3):
        mb = m.astype(jnp.bfloat16)
        m = jnp.dot(mb, mb, preferred_element_type=f32)
        n = norm(m)
        m = m / n
        root = n
        for _ in range(power + 1):
            root = jnp.sqrt(root)
        est = est * root
    size[...] = jnp.broadcast_to(est, size.shape)


class Line:
    def __init__(self, p):
        idx = here()
        self.p = p
        self.lane = lax.broadcasted_iota(jnp.int32, (SUB, p.nx), 1)
        self.idx = idx
        x = p.cols * idx[0] - p.hx + self.lane % p.wid
        self.xin = (x >= 0) & (x < p.nx)
        self.xown = (self.lane % p.wid >= p.hx) & (self.lane % p.wid < p.hx + p.cols)

    def ywin(self, s):
        return (self.lane // self.p.wid) * self.p.slabs + s

    def inside(self, s):
        p = self.p
        y = p.ny * self.idx[1] - p.depth + self.ywin(s)
        return self.xin & (y >= 0) & (y < p.ny * p.ngy)

    def own(self, s):
        p = self.p
        return self.xown & (self.ywin(s) >= p.depth) & (self.ywin(s) < p.depth + p.ny)

    def edges(self, ref):
        p = self.p
        for s in range(p.slabs + 2):
            ref[s, pl.ds(0, SUB), :] = jnp.zeros((SUB, p.nx), f32)
            ref[s, pl.ds(SUB + p.NZ, SUB), :] = jnp.zeros((SUB, p.nx), f32)

    def wrap(self, ref):
        p = self.p
        rows = pl.ds(SUB, p.NZ)
        ref[0, rows, :] = pltpu.roll(ref[p.slabs, rows, :], p.wid, 1)
        ref[p.slabs + 1, rows, :] = pltpu.roll(ref[1, rows, :], p.nx - p.wid, 1)

    def spread(self, recv, put):
        p = self.p
        for s in range(p.slabs):
            keep = self.inside(s)
            for j in range(p.ngx):
                for zt in range(p.nz // SUB):
                    got = recv[j, pl.ds(s * p.nz + zt * SUB, SUB), :]
                    put(s, j * p.nz + zt * SUB, jnp.where(keep, got, 0.0))

    def tile_of(self, ref, s, z):
        return lambda dz, dy: ref[s + 1 + dy, pl.ds(SUB + z + dz, SUB), :]


def line_kernel(plan, coup, recv, C, CS, G):
    p = plan
    nx = p.nx
    geo = Line(p)
    ki = [coup[0, k] for k in range(9)]
    geo.edges(G)

    def put(s, z, val):
        C[s, pl.ds(z, SUB), :] = val
        G[s + 1, pl.ds(SUB + z, SUB), :] = val

    geo.spread(recv, put)
    geo.wrap(G)
    step = TILES * SUB
    for s in range(p.slabs):

        def weigh(t, carry, s=s):
            vals = []
            for k in range(TILES):
                z = pl.multiple_of(t * step, step) + k * SUB
                vals.append((z, C[s, pl.ds(z, SUB), :] * combine(geo.tile_of(G, s, z), ki, None, None, nx)))
            for z, v in vals:
                CS[s, pl.ds(z, SUB), :] = v
            return carry

        lax.fori_loop(0, p.NZ // step, weigh, 0)


def basis_kernel(plan, coup, recv, factor, size, C, CS, basis, sums, G, W, B0, B1, B2, R0, BB):
    p = plan
    nx, off = p.nx, SUB
    geo = Line(p)
    wrap, tile_of, inside, own = geo.wrap, geo.tile_of, geo.inside, geo.own
    ki = [coup[0, k] for k in range(9)]
    ke = [coup[1, k] for k in range(9)]
    ki_sum, ke_sum = ki[0], ke[0]
    for k in range(1, 9):
        ki_sum = ki_sum + ki[k]
        ke_sum = ke_sum + ke[k]
    lam = 2.0 * (ki_sum + ke_sum) * size[...]
    quarter = 4.0 / lam
    ke_twice = 2.0 * ke_sum
    step = TILES * SUB
    geo.edges(G)
    geo.edges(W)

    def put(s, z, val):
        B0[s, pl.ds(z, SUB), :] = val
        R0[s, pl.ds(z, SUB), :] = val

    geo.spread(recv, put)

    ring = [B0, B1, B2]
    out = jnp.zeros((1, nx), f32)

    def lane_put(out, acc, at):
        v = jnp.sum(jnp.sum(acc, axis=1, keepdims=True), axis=0, keepdims=True)
        return jnp.where(lax.broadcasted_iota(jnp.int32, (1, nx), 1) == at, v, out)

    zero = jnp.zeros((SUB, nx), f32)
    slot = p.depth
    for j in range(p.depth):
        cur = ring[j % 3]
        prev = ring[(j + 2) % 3]
        new = ring[(j + 1) % 3]
        for s in range(p.slabs):
            b = cur[s]
            high = b.astype(jnp.bfloat16)
            cols = pl.ds(s * nx, nx)
            BB[pl.ds(0, p.NZ), cols] = high
            BB[pl.ds(p.NZ, p.NZ), cols] = high
            BB[pl.ds(2 * p.NZ, p.NZ), cols] = (b - high.astype(f32)).astype(jnp.bfloat16)
        prod = jnp.dot(factor[...], BB[...], preferred_element_type=f32)
        for s in range(p.slabs):
            part = prod[:, s * nx : (s + 1) * nx]
            basis[j, s] = part
            W[s + 1, pl.ds(off, p.NZ), :] = part
            G[s + 1, pl.ds(off, p.NZ), :] = part * C[s]
        wrap(W)
        wrap(G)
        accs = [zero] * (j + 2)
        for s in range(p.slabs):
            keep = inside(s)

            def apply(t, carry, s=s, keep=keep, j=j, cur=cur, prev=prev, new=new):
                res = list(carry)
                stores = []
                for k in range(TILES):
                    z = pl.multiple_of(t * step, step) + k * SUB
                    rows = pl.ds(z, SUB)
                    w = W[s + 1, pl.ds(off + z, SUB), :]
                    inner = combine(tile_of(G, s, z), ki, None, None, nx)
                    outer = combine(tile_of(W, s, z), ke, None, None, nx)
                    e = (CS[s, rows, :] + ke_twice) * w - C[s, rows, :] * inner - outer
                    e = jnp.where(keep, e, 0.0)
                    if j < p.depth - 1:
                        b = cur[s, rows, :]
                        if j == 0:
                            stores.append((rows, 0.5 * quarter * e - b))
                        else:
                            stores.append((rows, quarter * e - 2.0 * b - prev[s, rows, :]))
                    for i in range(j):
                        res[i] = res[i] + basis[i, s, rows, :] * e
                    res[j] = res[j] + w * e
                    res[j + 1] = res[j + 1] + w * R0[s, rows, :]
                for rows, value in stores:
                    new[s, rows, :] = value
                return tuple(res)

            got = lax.fori_loop(0, p.NZ // step, apply, tuple([zero] * (j + 2)))
            mine = own(s)
            accs = [a + jnp.where(mine, g, 0.0) for a, g in zip(accs, got)]
        out = lane_put(out, accs[j + 1], j)
        for i in range(j + 1):
            out = lane_put(out, accs[i], slot)
            slot += 1
    sums[...] = jnp.broadcast_to(out, sums.shape)


def solve_kernel(plan, recv, basis, send):
    p = plan
    nx, n = p.nx, p.depth
    tot = jnp.sum(recv[...], axis=0, keepdims=True)

    def get(k):
        return jnp.broadcast_to(tot[:, k : k + 1], (SUB, nx))

    rhs = [get(j) for j in range(n)]
    A = [[None] * n for _ in range(n)]
    slot = n
    for j in range(n):
        for i in range(j + 1):
            A[i][j] = A[j][i] = get(slot)
            slot += 1
    diag = [A[i][i] for i in range(n)]
    inv = [None] * n
    for k in range(n):
        ok = A[k][k] > 1e-7 * diag[k]
        inv[k] = jnp.where(ok, 1.0 / jnp.where(ok, A[k][k], 1.0), 0.0)
        for i in range(k + 1, n):
            m = A[i][k] * inv[k]
            for l in range(k + 1, n):
                A[i][l] = A[i][l] - m * A[k][l]
            rhs[i] = rhs[i] - m * rhs[k]
    sol = [None] * n
    for k in reversed(range(n)):
        acc = rhs[k]
        for l in range(k + 1, n):
            acc = acc - A[k][l] * sol[l]
        sol[k] = acc * inv[k]

    lane = lax.broadcasted_iota(jnp.int32, (SUB, nx), 1)
    group = lane // p.cols
    per = p.nz // SUB

    def pack(t, carry):
        rows = pl.ds(pl.multiple_of(t * SUB, SUB), SUB)
        dst = t // per
        part = []
        for s in range(p.slabs):
            acc = sol[0] * basis[0, s, rows, :]
            for i in range(1, n):
                acc = acc + sol[i] * basis[i, s, rows, :]
            part.append(acc)
        for o in range(p.back):
            acc = None
            for q2 in range(p.back_grp):
                y = p.depth + o * p.back_grp + q2
                q, s = y // p.slabs, y % p.slabs
                amount = (p.cols * q2 - (p.wid * q + p.hx)) % nx
                piece = pltpu.roll(part[s], amount, 1) if amount else part[s]
                acc = piece if acc is None else jnp.where(group == q2, piece, acc)
            send[dst, pl.ds(pl.multiple_of(o * p.nz + (t % per) * SUB, SUB), SUB), :] = acc
        return carry

    lax.fori_loop(0, p.NZ // SUB, pack, 0, unroll=2)


def finish_kernel(plan, recv, pot, out):
    p = plan
    nx = p.nx
    lane = lax.broadcasted_iota(jnp.int32, (SUB, nx), 1)
    group = lane // p.cols
    fpot = pot.reshape(p.nz * p.ny, nx)
    fout = out.reshape(p.nz * p.ny, nx)
    for o in range(p.back):
        for zt in range(p.nz // SUB):
            src = [recv[j, pl.ds(o * p.nz + zt * SUB, SUB), :] for j in range(p.ngx)]
            for q2 in range(p.back_grp):
                acc = None
                for j in range(p.ngx):
                    amount = (p.cols * j - p.cols * q2) % nx
                    piece = pltpu.roll(src[j], amount, 1) if amount else src[j]
                    acc = piece if acc is None else jnp.where(group == j, piece, acc)
                rows = pl.ds(zt * SUB * p.ny + o * p.back_grp + q2, SUB, stride=p.ny)
                fout[rows, :] = fpot[rows, :] + acc


def bidomain_step(voltage, potential, tissue, gain, couplings, line_factor):
    ngx, ngy = lax.axis_size("gx"), lax.axis_size("gy")
    p = Plan(voltage.shape, ngx, ngy)
    nz, ny, nx = p.nz, p.ny, p.nx
    sds = jax.ShapeDtypeStruct

    def call(kernel, ins, outs, scratch=()):
        return pl.pallas_call(
            kernel,
            out_shape=outs,
            in_specs=ins,
            out_specs=[VMEM] * len(outs),
            scratch_shapes=list(scratch),
            compiler_params=pltpu.CompilerParams(vmem_limit_bytes=58 * 1024 * 1024),
        )

    ysends = [None] if p.swap else [1, -1]
    shapes, routes = [], []

    def pairs(dz, dy):
        res = []
        for a in range(ngx):
            for b in range(ngy):
                if dy is None:
                    tb = (b + 1) % 2
                else:
                    tb = b + dy
                if 0 <= a + dz < ngx and 0 <= tb < ngy:
                    res.append((a * ngy + b, (a + dz) * ngy + tb))
        return res

    for dy in ysends:
        shapes.append(sds((3, nz, p.hy, nx), f32))
        routes.append((0, dy))
    for hop, n in p.hops:
        for sign in (1, -1):
            shapes.append(sds((3, n, ny, nx), f32))
            routes.append((sign * hop, 0))
            for dy in ysends:
                shapes.append(sds((3, n, p.hy, nx), f32))
                routes.append((sign * hop, dy))

    cond, *pieces = call(
        lambda *a: prep_kernel(p, *a), [VMEM] * 4, [sds(voltage.shape, f32)] + shapes
    )(voltage, potential, tissue, gain)
    halos = []
    for x, r in zip(pieces, routes):
        halos.append(lax.ppermute(x, ("gx", "gy"), pairs(*r)))

    line = pltpu.VMEM((p.slabs, p.NZ, nx), f32)
    wide = pltpu.VMEM((p.slabs + 2, p.NZ + 2 * SUB, nx), f32)
    half = pltpu.VMEM((3 * p.NZ, p.slabs * nx), jnp.bfloat16)

    def swap_lines(x):
        return lax.all_to_all(x, "gx", split_axis=0, concat_axis=0, tiled=True)

    sides = halos[: len(ysends)]
    (send_c,) = call(
        lambda *a: cond_kernel(p, *a), [VMEM] * (1 + len(sides)), [sds((ngx, p.slabs * nz, nx), f32)]
    )(cond, *sides)
    recv_c = swap_lines(send_c)
    line_c, line_cs = call(
        lambda *a: line_kernel(p, *a), [SMEM, VMEM], [sds((p.slabs, p.NZ, nx), f32)] * 2, [wide]
    )(couplings, recv_c)

    n_line = line_factor.shape[0]
    parts, size = call(
        factor_kernel, [VMEM] * 2, [sds((n_line, 3 * n_line), jnp.bfloat16), sds((SUB, nx), f32)]
    )(line_factor, line_factor.T)

    ext = pltpu.VMEM((p.yrows, p.zrows, nx), f32)
    new_voltage, send = call(
        lambda *a: cheb_kernel(p, *a),
        [SMEM] + [VMEM] * (3 + len(halos)),
        [sds(voltage.shape, f32), sds((ngx, p.slabs * nz, nx), f32)],
        [ext] * 8,
    )(couplings, voltage, potential, cond, *halos)

    recv = swap_lines(send)
    basis, sums = call(
        lambda *a: basis_kernel(p, *a),
        [SMEM] + [VMEM] * 5,
        [sds((p.depth, p.slabs, p.NZ, nx), f32), sds((ngx * ngy, nx), f32)],
        [wide, wide, line, line, line, line, half],
    )(couplings, recv, parts, size, line_c, line_cs)

    shares = lax.all_to_all(
        sums.reshape(ngx * ngy, 1, nx), ("gx", "gy"), split_axis=0, concat_axis=0, tiled=True
    ).reshape(ngx * ngy, nx)

    (back,) = call(
        lambda *a: solve_kernel(p, *a), [VMEM] * 2, [sds((ngx, p.back * nz, nx), f32)]
    )(shares, basis)
    home = lax.all_to_all(back, "gx", split_axis=0, concat_axis=0, tiled=True)
    (new_potential,) = call(
        lambda *a: finish_kernel(p, *a), [VMEM] * 2, [sds(voltage.shape, f32)]
    )(home, potential)
    return new_voltage, new_potential


def solution(mesh):
    spec = P("gx", "gy", None)
    return jax.shard_map(
        bidomain_step,
        mesh=mesh,
        in_specs=(spec, spec, spec, spec, P(), P()),
        out_specs=(spec, spec),
        check_vma=False,
    )
```

```python
import jax
import jax.numpy as jnp
from jax import lax
from jax.experimental import pallas as pl
from jax.experimental.pallas import tpu as pltpu
from jax.sharding import PartitionSpec as P


CHEB = 8
ITERS = 4
SUB = 8
ROWS = 4
TILES = 8

time_step = 2.0
ionic_rate = 0.5
onset_level = 0.2
gain_top = 3.0625
f32 = jnp.float32
VMEM = pl.BlockSpec(memory_space=pltpu.VMEM)
SMEM = pl.BlockSpec(memory_space=pltpu.SMEM)


def up_to(n, m):
    return -(-n // m) * m


class Plan:
    def __init__(self, local_shape, ngx, ngy):
        self.nz, self.ny, self.nx = local_shape
        self.ngx, self.ngy = ngx, ngy
        self.depth = ITERS
        self.hz = CHEB + 1
        self.hy = up_to(CHEB + 1 + ITERS, SUB)
        self.swap = ngy == 2
        self.hops = []
        left, hop = self.hz, 1
        while left > 0:
            self.hops.append((hop, min(self.nz, left)))
            left -= self.nz
            hop += 1
        self.pad = up_to(ITERS + 1, SUB)
        self.ywin = self.ny + self.hy * (1 if self.swap else 2)
        self.yrows = self.ywin + 2 * self.pad
        self.zrows = up_to(max(self.hz - d + up_to(self.nz + 2 * d, SUB) + 1 for d in range(self.hz)), SUB)
        self.zrows = max(self.zrows, up_to(self.nz + 2 * self.hz, SUB))
        self.NZ = self.nz * ngx
        self.cols = self.nx // ngx
        self.wid = 1
        while self.wid < self.cols + 2 * self.depth:
            self.wid *= 2
        self.hx = (self.wid - self.cols) // 2
        self.grp = self.nx // self.wid
        self.slabs = -(-(self.ny + 2 * self.depth) // self.grp)
        self.back_grp = self.nx // self.cols
        self.back = self.ny // self.back_grp


def here():
    return lax.axis_index("gx"), lax.axis_index("gy")


def prep_kernel(plan, volt_hbm, pot_hbm, tissue_hbm, gain_hbm, volt, pot, cond, *rest):
    *outs, tissue, gain, sems = rest
    idx = here()
    moves = [
        pltpu.make_async_copy(src, dst, sems.at[i])
        for i, (src, dst) in enumerate(
            ((tissue_hbm, tissue), (gain_hbm, gain), (volt_hbm, volt), (pot_hbm, pot))
        )
    ]
    for move in moves:
        move.start()
    moves[0].wait()
    moves[1].wait()
    cond[...] = tissue[...].astype(f32) * gain[...]
    moves[2].wait()
    moves[3].wait()
    fields = (volt, pot, cond)
    if plan.swap:
        ys = [pl.multiple_of((1 - idx[1]) * (plan.ny - plan.hy), SUB)]
    else:
        ys = [plan.ny - plan.hy, 0]
    at = 0
    for y0 in ys:
        for f, ref in enumerate(fields):
            outs[at][f] = ref[:, pl.ds(y0, plan.hy), :]
        at += 1
    for _, n in plan.hops:
        for z0 in (plan.nz - n, 0):
            for f, ref in enumerate(fields):
                outs[at][f] = ref[pl.ds(z0, n)]
            at += 1
            for y0 in ys:
                for f, ref in enumerate(fields):
                    outs[at][f] = ref[pl.ds(z0, n), pl.ds(y0, plan.hy), :]
                at += 1


def mixed(k):
    k = list(k)
    return k[:5] + [0.5 * (k[5] + k[6]), 0.5 * (k[5] - k[6]), 0.5 * (k[7] + k[8]), 0.5 * (k[7] - k[8])]


def combine(tile, k, left, right, width):
    mid, zp, zm, yp, ym = tile(0, 0), tile(1, 0), tile(-1, 0), tile(0, 1), tile(0, -1)
    zpyp, zmym, zpym, zmyp = tile(1, 1), tile(-1, -1), tile(1, -1), tile(-1, 1)
    zs, ys = zp + zm, yp + ym
    same = (k[0] * zs + k[1] * ys) + (k[3] * (zpyp + zmym) + k[4] * (zpym + zmyp))
    even = k[2] * mid + (k[5] * zs + k[7] * ys)
    odd = k[6] * (zp - zm) + k[8] * (yp - ym)
    plus = pltpu.roll(even + odd, width - 1, 1)
    minus = pltpu.roll(even - odd, 1, 1)
    if left is not None:
        plus = jnp.where(right, 0.0, plus)
        minus = jnp.where(left, 0.0, minus)
    return same + (plus + minus)


def cheb_kernel(plan, coup, volt, pot, cond, *rest):
    p = plan
    idx = here()
    ny_halo = 1 if p.swap else 2
    n_in = ny_halo + len(p.hops) * 2 * (1 + ny_halo)
    halos = rest[:n_in]
    new_volt, send = rest[n_in : n_in + 2]
    C, G0, G1, E, PT, R, U, D, C2 = rest[n_in + 2 :]
    nx = p.nx
    flat = lambda ref: ref.reshape(p.yrows * p.zrows, nx)
    if p.swap:
        ylocal = p.pad + idx[1] * p.hy
        yhalo = [p.pad + (1 - idx[1]) * p.ny]
    else:
        ylocal = p.pad + p.hy
        yhalo = [p.pad, p.pad + p.hy + p.ny]

    zero_rows = jnp.zeros((p.pad, p.zrows, nx), f32)
    for ref in (C, G0, G1, E, PT, R, U, D, C2):
        ref[pl.ds(0, p.pad)] = zero_rows
        ref[pl.ds(p.pad + p.ywin, p.pad)] = zero_rows

    fc, fg, fe, fp, fr = (flat(r) for r in (C, G0, E, PT, R))

    def place(getter, planes, zrow0, yrow0, ycount):
        def one(z, carry):
            for t in range(ycount // SUB):
                v, q, c = getter(z, t)
                start = (yrow0 + t * SUB) * p.zrows + zrow0 + z
                rows = pl.ds(start, SUB, stride=p.zrows)
                s = v + q
                mask = jnp.where(c > 0.0, 1.0, 0.0)
                fc[rows, :] = c
                fg[rows, :] = c * s
                fe[rows, :] = s
                fp[rows, :] = q
                fr[rows, :] = (-ionic_rate) * mask * v * (v - onset_level) * (v - 1.0)
            return carry

        lax.fori_loop(0, planes, one, 0)

    def local(z, t):
        ys = pl.ds(t * SUB, SUB)
        return volt[z, ys, :], pot[z, ys, :], cond[z, ys, :]

    def piece(ref):
        def get(z, t):
            ys = pl.ds(t * SUB, SUB)
            return ref[0, z, ys, :], ref[1, z, ys, :], ref[2, z, ys, :]

        return get

    place(local, p.nz, p.hz, ylocal, p.ny)
    at = 0
    for y0 in yhalo:
        place(piece(halos[at]), p.nz, p.hz, y0, p.hy)
        at += 1
    done = 0
    for _, n in p.hops:
        for z0 in (p.hz - done - n, p.hz + p.nz + done):
            place(piece(halos[at]), n, z0, ylocal, p.ny)
            at += 1
            for y0 in yhalo:
                place(piece(halos[at]), n, z0, y0, p.hy)
                at += 1
        done += n

    lane = lax.broadcasted_iota(jnp.int32, (SUB, nx), 1)
    left, right = lane == 0, lane == nx - 1
    ki = [coup[0, k] for k in range(9)]
    ke = [coup[1, k] for k in range(9)]
    total, ke_sum = ki[0], ke[0]
    for k in range(1, 9):
        total = total + ki[k]
        ke_sum = ke_sum + ke[k]
    ke_sum = 2.0 * ke_sum
    ki, ke = mixed(ki), mixed(ke)
    top = 1.0 + time_step * 4.0 * gain_top * jnp.full((SUB, nx), total, f32)
    centre = (top + 1.0) / 2.0
    half = (top - 1.0) / 2.0
    ratio = centre / half
    weight = 1.0 / ratio
    inv_centre = 1.0 / centre

    def sweep(d, body):
        tiles = up_to(p.nz + 2 * d, SUB) // SUB
        over = p.hy - p.depth - d
        y0 = p.pad + (idx[1] * over if p.swap else over)
        count = p.ny + (d + p.depth) * (1 if p.swap else 2)

        def block(i, carry):
            stores = []
            for r in range(ROWS):
                for t in range(tiles):
                    stores += body(y0 + i * ROWS + r, p.hz - d + t * SUB)
            for ref, where, value in stores:
                ref[where] = value
            return carry

        lax.fori_loop(0, -(-count // ROWS), block, 0)

    def tile_of(ref, y, z):
        return lambda dz, dy: ref[y + dy, pl.ds(z + dz, SUB), :]

    def first(y, z):
        rows = pl.ds(z, SUB)
        c = C[y, rows, :]
        s = E[y, rows, :]
        c2 = time_step * c
        cs = c2 * combine(tile_of(C, y, z), ki, left, right, nx)
        r = R[y, rows, :] - (cs * s - c2 * combine(tile_of(G0, y, z), ki, left, right, nx))
        u = r * inv_centre
        at = (y, rows)
        return [(D, at, 1.0 + cs), (C2, at, c2), (R, at, r), (U, at, u), (E, at, s + u), (G1, at, c * u)]

    sweep(CHEB, first)
    bufs = [G0, G1]
    for k in range(1, CHEB):
        gin, gout = bufs[k % 2], bufs[(k + 1) % 2]
        nxt = 1.0 / (2.0 * ratio - weight)
        keep, add = nxt * weight, 2.0 * nxt / half
        weight = nxt
        last = k == CHEB - 1

        def step(y, z, gin=gin, gout=gout, keep=keep, add=add, last=last):
            rows = pl.ds(z, SUB)
            c = C[y, rows, :]
            u = U[y, rows, :]
            flow = D[y, rows, :] * u - C2[y, rows, :] * combine(tile_of(gin, y, z), ki, left, right, nx)
            r = R[y, rows, :] - flow
            u = keep * u + add * r
            e = E[y, rows, :] + u
            at = (y, rows)
            if last:
                return [(E, at, e), (gout, at, c * e)]
            return [(E, at, e), (R, at, r), (U, at, u), (gout, at, c * u)]

        sweep(CHEB - k, step)

    gin = bufs[CHEB % 2]

    def final(y, z):
        rows = pl.ds(z, SUB)
        e = E[y, rows, :]
        flow = (D[y, rows, :] - 1.0) * e - C2[y, rows, :] * combine(tile_of(gin, y, z), ki, left, right, nx)
        outer = ke_sum * PT[y, rows, :] - combine(tile_of(PT, y, z), ke, left, right, nx)
        return [(R, (y, rows), (-1.0 / time_step) * flow - outer)]

    sweep(0, final)

    def give(z, carry):
        for t in range(p.ny // SUB):
            start = (ylocal + t * SUB) * p.zrows + p.hz + z
            rows = pl.ds(start, SUB, stride=p.zrows)
            new_volt[z, pl.ds(t * SUB, SUB), :] = fe[rows, :] - fp[rows, :]
        return carry

    lax.fori_loop(0, p.nz, give, 0)

    first_row = ylocal - p.depth

    def pack(s, carry):
        for zt in range(p.nz // SUB):
            rows = pl.ds(p.hz + zt * SUB, SUB)
            src = [R[first_row + q * p.slabs + s, rows, :] for q in range(p.grp)]
            windows(p, src, send, pl.multiple_of(s * p.nz + zt * SUB, SUB))
        return carry

    lax.fori_loop(0, p.slabs, pack, 0)


def windows(p, src, send, row):
    group = lax.broadcasted_iota(jnp.int32, (SUB, p.nx), 1) // p.wid
    for j in range(p.ngx):
        acc = None
        for q in range(p.grp):
            amount = (p.wid * q - (p.cols * j - p.hx)) % p.nx
            part = pltpu.roll(src[q], amount, 1) if amount else src[q]
            acc = part if acc is None else jnp.where(group == q, part, acc)
        send[j, pl.ds(row, SUB), :] = acc


def cond_kernel(plan, cond, *rest):
    p = plan
    *sides, send = rest
    idx = here()
    flat = cond.reshape(p.nz * p.ny, p.nx)
    flats = [ref.reshape(3 * p.nz * p.hy, p.nx) for ref in sides]

    def row_of(y, zt):
        if 0 <= y < p.ny:
            return flat[pl.ds(zt * SUB * p.ny + y, SUB, stride=p.ny), :]
        low = y < 0
        at = p.hy + y if low else y - p.ny
        if at >= p.hy:
            return jnp.zeros((SUB, p.nx), f32)
        ref = flats[0] if low else flats[-1]
        val = ref[pl.ds((2 * p.nz + zt * SUB) * p.hy + at, SUB, stride=p.hy), :]
        if p.swap:
            val = jnp.where(idx[1] == (1 if low else 0), val, 0.0)
        return val

    for s in range(p.slabs):
        for zt in range(p.nz // SUB):
            src = [row_of(q * p.slabs + s - p.depth, zt) for q in range(p.grp)]
            windows(p, src, send, s * p.nz + zt * SUB)


def factor_kernel(line, line_t, parts, size):
    scale = 1.0 / jnp.max(jnp.abs(line[...]), keepdims=True)
    a = line_t[...] * scale
    b = line[...] * scale
    g = jnp.dot(a, b, precision=lax.Precision.HIGHEST, preferred_element_type=f32)
    high = g.astype(jnp.bfloat16)
    n = g.shape[0]
    parts[:, pl.ds(0, n)] = high
    parts[:, pl.ds(n, n)] = (g - high.astype(f32)).astype(jnp.bfloat16)
    parts[:, pl.ds(2 * n, n)] = high

    def norm(m):
        return jnp.sqrt(jnp.sum(jnp.sum(m * m, axis=0, keepdims=True), axis=1, keepdims=True))

    n = norm(g)
    est = n
    m = g / n
    for power in range(3):
        mb = m.astype(jnp.bfloat16)
        m = jnp.dot(mb, mb, preferred_element_type=f32)
        n = norm(m)
        m = m / n
        root = n
        for _ in range(power + 1):
            root = jnp.sqrt(root)
        est = est * root
    size[...] = jnp.broadcast_to(est, size.shape)


class Line:
    def __init__(self, p):
        idx = here()
        self.p = p
        self.lane = lax.broadcasted_iota(jnp.int32, (SUB, p.nx), 1)
        self.idx = idx
        x = p.cols * idx[0] - p.hx + self.lane % p.wid
        self.xin = (x >= 0) & (x < p.nx)
        self.xown = (self.lane % p.wid >= p.hx) & (self.lane % p.wid < p.hx + p.cols)

    def ywin(self, s):
        return (self.lane // self.p.wid) * self.p.slabs + s

    def inside(self, s):
        p = self.p
        y = p.ny * self.idx[1] - p.depth + self.ywin(s)
        return self.xin & (y >= 0) & (y < p.ny * p.ngy)

    def own(self, s):
        p = self.p
        return self.xown & (self.ywin(s) >= p.depth) & (self.ywin(s) < p.depth + p.ny)

    def edges(self, ref):
        p = self.p
        for s in range(p.slabs + 2):
            ref[s, pl.ds(0, SUB), :] = jnp.zeros((SUB, p.nx), f32)
            ref[s, pl.ds(SUB + p.NZ, SUB), :] = jnp.zeros((SUB, p.nx), f32)

    def wrap(self, ref):
        p = self.p
        rows = pl.ds(SUB, p.NZ)
        ref[0, rows, :] = pltpu.roll(ref[p.slabs, rows, :], p.wid, 1)
        ref[p.slabs + 1, rows, :] = pltpu.roll(ref[1, rows, :], p.nx - p.wid, 1)

    def spread(self, recv, put):
        p = self.p
        for s in range(p.slabs):
            keep = self.inside(s)
            for j in range(p.ngx):
                for zt in range(p.nz // SUB):
                    got = recv[j, pl.ds(s * p.nz + zt * SUB, SUB), :]
                    put(s, j * p.nz + zt * SUB, jnp.where(keep, got, 0.0))

    def tile_of(self, ref, s, z):
        return lambda dz, dy: ref[s + 1 + dy, pl.ds(SUB + z + dz, SUB), :]


def line_kernel(plan, coup, recv, C, CS, G):
    p = plan
    nx = p.nx
    geo = Line(p)
    ki = mixed([coup[0, k] for k in range(9)])
    ke_sum = coup[1, 0]
    for k in range(1, 9):
        ke_sum = ke_sum + coup[1, k]
    ke_twice = 2.0 * ke_sum
    geo.edges(G)

    def put(s, z, val):
        C[s, pl.ds(z, SUB), :] = val
        G[s + 1, pl.ds(SUB + z, SUB), :] = val

    geo.spread(recv, put)
    geo.wrap(G)
    step = TILES * SUB
    for s in range(p.slabs):

        def weigh(t, carry, s=s):
            vals = []
            for k in range(TILES):
                z = pl.multiple_of(t * step, step) + k * SUB
                part = combine(geo.tile_of(G, s, z), ki, None, None, nx)
                vals.append((z, ke_twice + C[s, pl.ds(z, SUB), :] * part))
            for z, v in vals:
                CS[s, pl.ds(z, SUB), :] = v
            return carry

        lax.fori_loop(0, p.NZ // step, weigh, 0)


def basis_kernel(plan, coup, recv, factor, size, C, CS, basis, sums, G, W, B0, B1, B2, R0, BB):
    p = plan
    nx, off = p.nx, SUB
    geo = Line(p)
    wrap, tile_of, inside, own = geo.wrap, geo.tile_of, geo.inside, geo.own
    ki = [coup[0, k] for k in range(9)]
    ke = [coup[1, k] for k in range(9)]
    ki_sum, ke_sum = ki[0], ke[0]
    for k in range(1, 9):
        ki_sum = ki_sum + ki[k]
        ke_sum = ke_sum + ke[k]
    lam = 2.0 * (ki_sum + ke_sum) * size[...]
    quarter = 4.0 / lam
    ki, ke = mixed(ki), mixed(ke)
    step = TILES * SUB
    geo.edges(G)
    geo.edges(W)

    def put(s, z, val):
        B0[s, pl.ds(z, SUB), :] = val
        R0[s, pl.ds(z, SUB), :] = val

    geo.spread(recv, put)

    ring = [B0, B1, B2]
    out = jnp.zeros((1, nx), f32)

    def lane_put(out, acc, at):
        v = jnp.sum(jnp.sum(acc, axis=1, keepdims=True), axis=0, keepdims=True)
        return jnp.where(lax.broadcasted_iota(jnp.int32, (1, nx), 1) == at, v, out)

    zero = jnp.zeros((SUB, nx), f32)
    slot = p.depth
    for j in range(p.depth):
        cur = ring[j % 3]
        prev = ring[(j + 2) % 3]
        new = ring[(j + 1) % 3]
        for s in range(p.slabs):
            b = cur[s]
            high = b.astype(jnp.bfloat16)
            cols = pl.ds(s * nx, nx)
            BB[pl.ds(0, p.NZ), cols] = high
            BB[pl.ds(p.NZ, p.NZ), cols] = high
            BB[pl.ds(2 * p.NZ, p.NZ), cols] = (b - high.astype(f32)).astype(jnp.bfloat16)
        prod = jnp.dot(factor[...], BB[...], preferred_element_type=f32)
        for s in range(p.slabs):
            part = prod[:, s * nx : (s + 1) * nx]
            basis[j, s] = part
            W[s + 1, pl.ds(off, p.NZ), :] = part
            G[s + 1, pl.ds(off, p.NZ), :] = part * C[s]
        wrap(W)
        wrap(G)
        accs = [zero] * (j + 2)
        for s in range(p.slabs):
            keep = inside(s)

            def apply(t, carry, s=s, keep=keep, j=j, cur=cur, prev=prev, new=new):
                res = list(carry)
                stores = []
                for k in range(TILES):
                    z = pl.multiple_of(t * step, step) + k * SUB
                    rows = pl.ds(z, SUB)
                    w = W[s + 1, pl.ds(off + z, SUB), :]
                    inner = combine(tile_of(G, s, z), ki, None, None, nx)
                    outer = combine(tile_of(W, s, z), ke, None, None, nx)
                    e = CS[s, rows, :] * w - C[s, rows, :] * inner - outer
                    e = jnp.where(keep, e, 0.0)
                    if j < p.depth - 1:
                        b = cur[s, rows, :]
                        if j == 0:
                            stores.append((rows, 0.5 * quarter * e - b))
                        else:
                            stores.append((rows, quarter * e - 2.0 * b - prev[s, rows, :]))
                    for i in range(j):
                        res[i] = res[i] + basis[i, s, rows, :] * e
                    res[j] = res[j] + w * e
                    res[j + 1] = res[j + 1] + w * R0[s, rows, :]
                for rows, value in stores:
                    new[s, rows, :] = value
                return tuple(res)

            got = lax.fori_loop(0, p.NZ // step, apply, tuple([zero] * (j + 2)))
            mine = own(s)
            accs = [a + jnp.where(mine, g, 0.0) for a, g in zip(accs, got)]
        out = lane_put(out, accs[j + 1], j)
        for i in range(j + 1):
            out = lane_put(out, accs[i], slot)
            slot += 1
    sums[...] = jnp.broadcast_to(out, sums.shape)


def solve_kernel(plan, recv, basis, send):
    p = plan
    nx, n = p.nx, p.depth
    tot = jnp.sum(recv[...], axis=0, keepdims=True)

    def get(k):
        return jnp.broadcast_to(tot[:, k : k + 1], (SUB, nx))

    rhs = [get(j) for j in range(n)]
    A = [[None] * n for _ in range(n)]
    slot = n
    for j in range(n):
        for i in range(j + 1):
            A[i][j] = A[j][i] = get(slot)
            slot += 1
    diag = [A[i][i] for i in range(n)]
    inv = [None] * n
    for k in range(n):
        ok = A[k][k] > 1e-7 * diag[k]
        inv[k] = jnp.where(ok, 1.0 / jnp.where(ok, A[k][k], 1.0), 0.0)
        for i in range(k + 1, n):
            m = A[i][k] * inv[k]
            for l in range(k + 1, n):
                A[i][l] = A[i][l] - m * A[k][l]
            rhs[i] = rhs[i] - m * rhs[k]
    sol = [None] * n
    for k in reversed(range(n)):
        acc = rhs[k]
        for l in range(k + 1, n):
            acc = acc - A[k][l] * sol[l]
        sol[k] = acc * inv[k]

    lane = lax.broadcasted_iota(jnp.int32, (SUB, nx), 1)
    group = lane // p.cols
    per = p.nz // SUB

    def pack(t, carry):
        rows = pl.ds(pl.multiple_of(t * SUB, SUB), SUB)
        dst = t // per
        part = []
        for s in range(p.slabs):
            acc = sol[0] * basis[0, s, rows, :]
            for i in range(1, n):
                acc = acc + sol[i] * basis[i, s, rows, :]
            part.append(acc)
        for o in range(p.back):
            acc = None
            for q2 in range(p.back_grp):
                y = p.depth + o * p.back_grp + q2
                q, s = y // p.slabs, y % p.slabs
                amount = (p.cols * q2 - (p.wid * q + p.hx)) % nx
                piece = pltpu.roll(part[s], amount, 1) if amount else part[s]
                acc = piece if acc is None else jnp.where(group == q2, piece, acc)
            send[dst, pl.ds(pl.multiple_of(o * p.nz + (t % per) * SUB, SUB), SUB), :] = acc
        return carry

    lax.fori_loop(0, p.NZ // SUB, pack, 0, unroll=2)


def finish_kernel(plan, recv, pot, out):
    p = plan
    nx = p.nx
    lane = lax.broadcasted_iota(jnp.int32, (SUB, nx), 1)
    group = lane // p.cols
    fpot = pot.reshape(p.nz * p.ny, nx)
    fout = out.reshape(p.nz * p.ny, nx)
    for o in range(p.back):
        for zt in range(p.nz // SUB):
            src = [recv[j, pl.ds(o * p.nz + zt * SUB, SUB), :] for j in range(p.ngx)]
            for q2 in range(p.back_grp):
                acc = None
                for j in range(p.ngx):
                    amount = (p.cols * j - p.cols * q2) % nx
                    piece = pltpu.roll(src[j], amount, 1) if amount else src[j]
                    acc = piece if acc is None else jnp.where(group == j, piece, acc)
                rows = pl.ds(zt * SUB * p.ny + o * p.back_grp + q2, SUB, stride=p.ny)
                fout[rows, :] = fpot[rows, :] + acc


def bidomain_step(voltage, potential, tissue, gain, couplings, line_factor):
    ngx, ngy = lax.axis_size("gx"), lax.axis_size("gy")
    p = Plan(voltage.shape, ngx, ngy)
    nz, ny, nx = p.nz, p.ny, p.nx
    sds = jax.ShapeDtypeStruct

    def call(kernel, ins, outs, scratch=(), mib=12):
        return pl.pallas_call(
            kernel,
            out_shape=outs,
            in_specs=ins,
            out_specs=[VMEM] * len(outs),
            scratch_shapes=list(scratch),
            compiler_params=pltpu.CompilerParams(vmem_limit_bytes=mib * 1024 * 1024),
        )

    ysends = [None] if p.swap else [1, -1]
    shapes, routes = [], []

    def pairs(dz, dy):
        res = []
        for a in range(ngx):
            for b in range(ngy):
                if dy is None:
                    tb = (b + 1) % 2
                else:
                    tb = b + dy
                if 0 <= a + dz < ngx and 0 <= tb < ngy:
                    res.append((a * ngy + b, (a + dz) * ngy + tb))
        return res

    for dy in ysends:
        shapes.append(sds((3, nz, p.hy, nx), f32))
        routes.append((0, dy))
    for hop, n in p.hops:
        for sign in (1, -1):
            shapes.append(sds((3, n, ny, nx), f32))
            routes.append((sign * hop, 0))
            for dy in ysends:
                shapes.append(sds((3, n, p.hy, nx), f32))
                routes.append((sign * hop, dy))

    volt, pot, cond, *pieces = call(
        lambda *a: prep_kernel(p, *a),
        [pl.BlockSpec(memory_space=pltpu.HBM)] * 4,
        [sds(voltage.shape, f32)] * 3 + shapes,
        [pltpu.VMEM(voltage.shape, jnp.int32), pltpu.VMEM(voltage.shape, f32), pltpu.SemaphoreType.DMA((4,))],
    )(*(pltpu.with_memory_space_constraint(x, pltpu.HBM) for x in (voltage, potential, tissue, gain)))
    halos = []
    for x, r in zip(pieces, routes):
        halos.append(lax.ppermute(x, ("gx", "gy"), pairs(*r)))

    line = pltpu.VMEM((p.slabs, p.NZ, nx), f32)
    wide = pltpu.VMEM((p.slabs + 2, p.NZ + 2 * SUB, nx), f32)
    half = pltpu.VMEM((3 * p.NZ, p.slabs * nx), jnp.bfloat16)

    def swap_lines(x):
        return lax.all_to_all(x, "gx", split_axis=0, concat_axis=0, tiled=True)

    sides = halos[: len(ysends)]
    (send_c,) = call(
        lambda *a: cond_kernel(p, *a), [VMEM] * (1 + len(sides)), [sds((ngx, p.slabs * nz, nx), f32)]
    )(cond, *sides)
    recv_c = swap_lines(send_c)
    line_c, line_cs = call(
        lambda *a: line_kernel(p, *a), [SMEM, VMEM], [sds((p.slabs, p.NZ, nx), f32)] * 2, [wide]
    )(couplings, recv_c)

    n_line = line_factor.shape[0]
    parts, size = call(
        factor_kernel, [VMEM] * 2, [sds((n_line, 3 * n_line), jnp.bfloat16), sds((SUB, nx), f32)]
    )(line_factor, line_factor.T)

    ext = pltpu.VMEM((p.yrows, p.zrows, nx), f32)
    new_voltage, send = call(
        lambda *a: cheb_kernel(p, *a),
        [SMEM] + [VMEM] * (3 + len(halos)),
        [sds(voltage.shape, f32), sds((ngx, p.slabs * nz, nx), f32)],
        [ext] * 9,
        mib=24,
    )(couplings, volt, pot, cond, *halos)

    recv = swap_lines(send)
    basis, sums = call(
        lambda *a: basis_kernel(p, *a),
        [SMEM] + [VMEM] * 5,
        [sds((p.depth, p.slabs, p.NZ, nx), f32), sds((ngx * ngy, nx), f32)],
        [wide, wide, line, line, line, line, half],
        mib=24,
    )(couplings, recv, parts, size, line_c, line_cs)

    shares = lax.all_to_all(
        sums.reshape(ngx * ngy, 1, nx), ("gx", "gy"), split_axis=0, concat_axis=0, tiled=True
    ).reshape(ngx * ngy, nx)

    (back,) = call(
        lambda *a: solve_kernel(p, *a), [VMEM] * 2, [sds((ngx, p.back * nz, nx), f32)]
    )(shares, basis)
    home = lax.all_to_all(back, "gx", split_axis=0, concat_axis=0, tiled=True)
    (new_potential,) = call(
        lambda *a: finish_kernel(p, *a), [VMEM] * 2, [sds(voltage.shape, f32)]
    )(home, pot)
    return new_voltage, new_potential


def solution(mesh):
    spec = P("gx", "gy", None)
    return jax.shard_map(
        bidomain_step,
        mesh=mesh,
        in_specs=(spec, spec, spec, spec, P(), P()),
        out_specs=(spec, spec),
        check_vma=False,
    )
```

```python
import jax
import jax.numpy as jnp
from jax import lax
from jax.experimental import pallas as pl
from jax.experimental.pallas import tpu as pltpu
from jax.sharding import PartitionSpec as P


CHEB = 8
ITERS = 4
SUB = 8
TRIP = 48
TILES = 8

time_step = 2.0
ionic_rate = 0.5
onset_level = 0.2
gain_top = 3.0625
f32 = jnp.float32
VMEM = pl.BlockSpec(memory_space=pltpu.VMEM)
ANY = pl.BlockSpec(memory_space=pl.ANY)


def up_to(n, m):
    return -(-n // m) * m


class Plan:
    def __init__(self, local_shape, ngx, ngy):
        self.nz, self.ny, self.nx = local_shape
        self.ngx, self.ngy = ngx, ngy
        self.depth = ITERS
        self.hz = CHEB + 1
        self.hy = up_to(CHEB + 1 + ITERS, SUB)
        self.swap = ngy == 2
        self.hops = []
        left, hop = self.hz, 1
        while left > 0:
            self.hops.append((hop, min(self.nz, left)))
            left -= self.nz
            hop += 1
        self.pad = up_to(ITERS + 1, SUB)
        self.ywin = self.ny + self.hy * (1 if self.swap else 2)
        self.yrows = self.ywin + 2 * self.pad
        self.zrows = up_to(max(self.hz - d + up_to(self.nz + 2 * d, SUB) + 1 for d in range(self.hz)), SUB)
        self.zrows = max(self.zrows, up_to(self.nz + 2 * self.hz, SUB))
        self.NZ = self.nz * ngx
        self.cols = self.nx // ngx
        self.wid = 1
        while self.wid < self.cols + 2 * self.depth:
            self.wid *= 2
        self.hx = (self.wid - self.cols) // 2
        self.grp = self.nx // self.wid
        self.slabs = -(-(self.ny + 2 * self.depth) // self.grp)
        self.back_grp = self.nx // self.cols
        self.back = self.ny // self.back_grp


def here():
    return lax.axis_index("gx"), lax.axis_index("gy")


def block_rows(count, tiles):
    def cost(r):
        trips = -(-count // r)
        return trips * (150 + 9 * r * tiles) if trips * r - count < SUB - 1 else 1 << 30

    return min(range(1, max(2, TRIP // tiles + 1)), key=cost)


def prep_kernel(plan, volt_hbm, pot_hbm, tissue_hbm, gain_hbm, volt, pot, cond, *rest):
    *outs, tissue, gain, sems = rest
    idx = here()
    moves = [
        pltpu.make_async_copy(src, dst, sems.at[i])
        for i, (src, dst) in enumerate(
            ((tissue_hbm, tissue), (gain_hbm, gain), (volt_hbm, volt), (pot_hbm, pot))
        )
    ]
    for move in moves:
        move.start()
    moves[0].wait()
    moves[1].wait()
    cond[...] = tissue[...].astype(f32) * gain[...]
    moves[2].wait()
    moves[3].wait()
    fields = (volt, pot, cond)
    if plan.swap:
        ys = [pl.multiple_of((1 - idx[1]) * (plan.ny - plan.hy), SUB)]
    else:
        ys = [plan.ny - plan.hy, 0]
    at = 0
    for y0 in ys:
        for f, ref in enumerate(fields):
            outs[at][f] = ref[:, pl.ds(y0, plan.hy), :]
        at += 1
    for _, n in plan.hops:
        for z0 in (plan.nz - n, 0):
            for f, ref in enumerate(fields):
                outs[at][f] = ref[pl.ds(z0, n)]
            at += 1
            for y0 in ys:
                for f, ref in enumerate(fields):
                    outs[at][f] = ref[pl.ds(z0, n), pl.ds(y0, plan.hy), :]
                at += 1


def mixed(k):
    k = list(k)
    return k[:5] + [0.5 * (k[5] + k[6]), 0.5 * (k[5] - k[6]), 0.5 * (k[7] + k[8]), 0.5 * (k[7] - k[8])]


def combine(tile, k, left, right, width):
    mid, zp, zm, yp, ym = tile(0, 0), tile(1, 0), tile(-1, 0), tile(0, 1), tile(0, -1)
    zpyp, zmym, zpym, zmyp = tile(1, 1), tile(-1, -1), tile(1, -1), tile(-1, 1)
    zs, ys = zp + zm, yp + ym
    same = (k[0] * zs + k[1] * ys) + (k[3] * (zpyp + zmym) + k[4] * (zpym + zmyp))
    even = k[2] * mid + (k[5] * zs + k[7] * ys)
    odd = k[6] * (zp - zm) + k[8] * (yp - ym)
    plus = pltpu.roll(even + odd, width - 1, 1)
    minus = pltpu.roll(even - odd, 1, 1)
    if left is not None:
        plus = jnp.where(right, 0.0, plus)
        minus = jnp.where(left, 0.0, minus)
    return same + (plus + minus)


def cheb_kernel(plan, coup_any, volt, pot, cond, *rest):
    p = plan
    idx = here()
    ny_halo = 1 if p.swap else 2
    n_in = ny_halo + len(p.hops) * 2 * (1 + ny_halo)
    halos = rest[:n_in]
    new_volt, send = rest[n_in : n_in + 2]
    C, G0, G1, E, PT, R, U, D, C2, coup, sem = rest[n_in + 2 :]
    move = pltpu.make_async_copy(coup_any, coup, sem)
    move.start()
    nx = p.nx
    flat = lambda ref: ref.reshape(p.yrows * p.zrows, nx)
    if p.swap:
        ylocal = p.pad + idx[1] * p.hy
        yhalo = [p.pad + (1 - idx[1]) * p.ny]
    else:
        ylocal = p.pad + p.hy
        yhalo = [p.pad, p.pad + p.hy + p.ny]

    zero_rows = jnp.zeros((p.pad, p.zrows, nx), f32)
    for ref in (C, G0, G1, E, PT, R, U, D, C2):
        ref[pl.ds(0, p.pad)] = zero_rows
        ref[pl.ds(p.pad + p.ywin, p.pad)] = zero_rows

    fc, fg, fe, fp, fr = (flat(r) for r in (C, G0, E, PT, R))

    def place(getter, planes, zrow0, yrow0, ycount):
        def one(z, carry):
            for t in range(ycount // SUB):
                v, q, c = getter(z, t)
                start = (yrow0 + t * SUB) * p.zrows + zrow0 + z
                rows = pl.ds(start, SUB, stride=p.zrows)
                s = v + q
                mask = jnp.where(c > 0.0, 1.0, 0.0)
                fc[rows, :] = c
                fg[rows, :] = c * s
                fe[rows, :] = s
                fp[rows, :] = q
                fr[rows, :] = (-ionic_rate) * mask * v * (v - onset_level) * (v - 1.0)
            return carry

        lax.fori_loop(0, planes, one, 0)

    def local(z, t):
        ys = pl.ds(t * SUB, SUB)
        return volt[z, ys, :], pot[z, ys, :], cond[z, ys, :]

    def piece(ref):
        def get(z, t):
            ys = pl.ds(t * SUB, SUB)
            return ref[0, z, ys, :], ref[1, z, ys, :], ref[2, z, ys, :]

        return get

    place(local, p.nz, p.hz, ylocal, p.ny)
    at = 0
    for y0 in yhalo:
        place(piece(halos[at]), p.nz, p.hz, y0, p.hy)
        at += 1
    done = 0
    for _, n in p.hops:
        for z0 in (p.hz - done - n, p.hz + p.nz + done):
            place(piece(halos[at]), n, z0, ylocal, p.ny)
            at += 1
            for y0 in yhalo:
                place(piece(halos[at]), n, z0, y0, p.hy)
                at += 1
        done += n

    lane = lax.broadcasted_iota(jnp.int32, (SUB, nx), 1)
    left, right = lane == 0, lane == nx - 1
    move.wait()
    ki = [coup[0, k] for k in range(9)]
    ke = [coup[1, k] for k in range(9)]
    total, ke_sum = ki[0], ke[0]
    for k in range(1, 9):
        total = total + ki[k]
        ke_sum = ke_sum + ke[k]
    ke_sum = 2.0 * ke_sum
    ki, ke = mixed(ki), mixed(ke)
    top = 1.0 + time_step * 4.0 * gain_top * jnp.full((SUB, nx), total, f32)
    centre = (top + 1.0) / 2.0
    half = (top - 1.0) / 2.0
    ratio = centre / half
    weight = 1.0 / ratio
    inv_centre = 1.0 / centre

    def sweep(d, body):
        tiles = up_to(p.nz + 2 * d, SUB) // SUB
        over = p.hy - p.depth - d
        y0 = p.pad + (idx[1] * over if p.swap else over)
        count = p.ny + (d + p.depth) * (1 if p.swap else 2)

        step = block_rows(count, tiles)

        def block(i, carry):
            stores = []
            for r in range(step):
                for t in range(tiles):
                    stores += body(y0 + i * step + r, p.hz - d + t * SUB)
            for ref, where, value in stores:
                ref[where] = value
            return carry

        lax.fori_loop(0, -(-count // step), block, 0)

    def tile_of(ref, y, z):
        return lambda dz, dy: ref[y + dy, pl.ds(z + dz, SUB), :]

    def first(y, z):
        rows = pl.ds(z, SUB)
        c = C[y, rows, :]
        s = E[y, rows, :]
        c2 = time_step * c
        cs = c2 * combine(tile_of(C, y, z), ki, left, right, nx)
        r = R[y, rows, :] - (cs * s - c2 * combine(tile_of(G0, y, z), ki, left, right, nx))
        u = r * inv_centre
        at = (y, rows)
        return [(D, at, 1.0 + cs), (C2, at, c2), (R, at, r), (U, at, u), (E, at, s + u), (G1, at, c * u)]

    sweep(CHEB, first)
    bufs = [G0, G1]
    for k in range(1, CHEB):
        gin, gout = bufs[k % 2], bufs[(k + 1) % 2]
        nxt = 1.0 / (2.0 * ratio - weight)
        keep, add = nxt * weight, 2.0 * nxt / half
        weight = nxt
        last = k == CHEB - 1

        def step(y, z, gin=gin, gout=gout, keep=keep, add=add, last=last):
            rows = pl.ds(z, SUB)
            c = C[y, rows, :]
            u = U[y, rows, :]
            flow = D[y, rows, :] * u - C2[y, rows, :] * combine(tile_of(gin, y, z), ki, left, right, nx)
            r = R[y, rows, :] - flow
            u = keep * u + add * r
            e = E[y, rows, :] + u
            at = (y, rows)
            if last:
                return [(E, at, e), (gout, at, c * e)]
            return [(E, at, e), (R, at, r), (U, at, u), (gout, at, c * u)]

        sweep(CHEB - k, step)

    gin = bufs[CHEB % 2]

    def final(y, z):
        rows = pl.ds(z, SUB)
        e = E[y, rows, :]
        flow = (D[y, rows, :] - 1.0) * e - C2[y, rows, :] * combine(tile_of(gin, y, z), ki, left, right, nx)
        outer = ke_sum * PT[y, rows, :] - combine(tile_of(PT, y, z), ke, left, right, nx)
        return [(R, (y, rows), (-1.0 / time_step) * flow - outer)]

    sweep(0, final)

    def give(z, carry):
        for t in range(p.ny // SUB):
            start = (ylocal + t * SUB) * p.zrows + p.hz + z
            rows = pl.ds(start, SUB, stride=p.zrows)
            new_volt[z, pl.ds(t * SUB, SUB), :] = fe[rows, :] - fp[rows, :]
        return carry

    lax.fori_loop(0, p.nz, give, 0)

    first_row = ylocal - p.depth

    def pack(s, carry):
        for zt in range(p.nz // SUB):
            rows = pl.ds(p.hz + zt * SUB, SUB)
            src = [R[first_row + q * p.slabs + s, rows, :] for q in range(p.grp)]
            windows(p, src, send, pl.multiple_of(s * p.nz + zt * SUB, SUB))
        return carry

    lax.fori_loop(0, p.slabs, pack, 0)


def windows(p, src, send, row):
    group = lax.broadcasted_iota(jnp.int32, (SUB, p.nx), 1) // p.wid
    for j in range(p.ngx):
        acc = None
        for q in range(p.grp):
            amount = (p.wid * q - (p.cols * j - p.hx)) % p.nx
            part = pltpu.roll(src[q], amount, 1) if amount else src[q]
            acc = part if acc is None else jnp.where(group == q, part, acc)
        send[j, pl.ds(row, SUB), :] = acc


def cond_kernel(plan, cond, *rest):
    p = plan
    *sides, send = rest
    idx = here()
    flat = cond.reshape(p.nz * p.ny, p.nx)
    flats = [ref.reshape(3 * p.nz * p.hy, p.nx) for ref in sides]

    def row_of(y, zt):
        if 0 <= y < p.ny:
            return flat[pl.ds(zt * SUB * p.ny + y, SUB, stride=p.ny), :]
        low = y < 0
        at = p.hy + y if low else y - p.ny
        if at >= p.hy:
            return jnp.zeros((SUB, p.nx), f32)
        ref = flats[0] if low else flats[-1]
        val = ref[pl.ds((2 * p.nz + zt * SUB) * p.hy + at, SUB, stride=p.hy), :]
        if p.swap:
            val = jnp.where(idx[1] == (1 if low else 0), val, 0.0)
        return val

    for s in range(p.slabs):
        for zt in range(p.nz // SUB):
            src = [row_of(q * p.slabs + s - p.depth, zt) for q in range(p.grp)]
            windows(p, src, send, s * p.nz + zt * SUB)


def factor_kernel(line, line_t, parts, size):
    scale = 1.0 / jnp.max(jnp.abs(line[...]), keepdims=True)
    a = line_t[...] * scale
    b = line[...] * scale
    g = jnp.dot(a, b, precision=lax.Precision.HIGHEST, preferred_element_type=f32)
    high = g.astype(jnp.bfloat16)
    n = g.shape[0]
    parts[:, pl.ds(0, n)] = high
    parts[:, pl.ds(n, n)] = (g - high.astype(f32)).astype(jnp.bfloat16)
    parts[:, pl.ds(2 * n, n)] = high

    def norm(m):
        return jnp.sqrt(jnp.sum(jnp.sum(m * m, axis=0, keepdims=True), axis=1, keepdims=True))

    n = norm(g)
    est = n
    m = g / n
    for power in range(3):
        mb = m.astype(jnp.bfloat16)
        m = jnp.dot(mb, mb, preferred_element_type=f32)
        n = norm(m)
        m = m / n
        root = n
        for _ in range(power + 1):
            root = jnp.sqrt(root)
        est = est * root
    size[...] = jnp.broadcast_to(est, size.shape)


class Line:
    def __init__(self, p):
        idx = here()
        self.p = p
        self.lane = lax.broadcasted_iota(jnp.int32, (SUB, p.nx), 1)
        self.idx = idx
        x = p.cols * idx[0] - p.hx + self.lane % p.wid
        self.xin = (x >= 0) & (x < p.nx)
        self.xown = (self.lane % p.wid >= p.hx) & (self.lane % p.wid < p.hx + p.cols)

    def ywin(self, s):
        return (self.lane // self.p.wid) * self.p.slabs + s

    def inside(self, s):
        p = self.p
        y = p.ny * self.idx[1] - p.depth + self.ywin(s)
        return self.xin & (y >= 0) & (y < p.ny * p.ngy)

    def own(self, s):
        p = self.p
        return self.xown & (self.ywin(s) >= p.depth) & (self.ywin(s) < p.depth + p.ny)

    def edges(self, ref):
        p = self.p
        for s in range(p.slabs + 2):
            ref[s, pl.ds(0, SUB), :] = jnp.zeros((SUB, p.nx), f32)
            ref[s, pl.ds(SUB + p.NZ, SUB), :] = jnp.zeros((SUB, p.nx), f32)

    def wrap(self, ref):
        p = self.p
        rows = pl.ds(SUB, p.NZ)
        ref[0, rows, :] = pltpu.roll(ref[p.slabs, rows, :], p.wid, 1)
        ref[p.slabs + 1, rows, :] = pltpu.roll(ref[1, rows, :], p.nx - p.wid, 1)

    def spread(self, recv, put):
        p = self.p

        def one(s, carry):
            keep = self.inside(s)
            for j in range(p.ngx):
                for zt in range(p.nz // SUB):
                    got = recv[j, pl.ds(pl.multiple_of(s * p.nz, SUB) + zt * SUB, SUB), :]
                    put(s, j * p.nz + zt * SUB, jnp.where(keep, got, 0.0))
            return carry

        lax.fori_loop(0, p.slabs, one, 0)

    def tile_of(self, ref, s, z):
        return lambda dz, dy: ref[s + 1 + dy, pl.ds(SUB + z + dz, SUB), :]


def line_kernel(plan, coup_any, recv, C, CS, G, coup, sem):
    p = plan
    nx = p.nx
    move = pltpu.make_async_copy(coup_any, coup, sem)
    move.start()
    geo = Line(p)
    geo.edges(G)

    def put(s, z, val):
        C[s, pl.ds(z, SUB), :] = val
        G[s + 1, pl.ds(SUB + z, SUB), :] = val

    geo.spread(recv, put)
    geo.wrap(G)
    move.wait()
    ki = mixed([coup[0, k] for k in range(9)])
    ke_sum = coup[1, 0]
    for k in range(1, 9):
        ke_sum = ke_sum + coup[1, k]
    ke_twice = 2.0 * ke_sum
    step = TILES * SUB

    def weigh(t, carry):
        vals = []
        for k in range(TILES):
            z = pl.multiple_of(t * step, step) + k * SUB
            for s in range(p.slabs):
                part = combine(geo.tile_of(G, s, z), ki, None, None, nx)
                vals.append((s, z, ke_twice + C[s, pl.ds(z, SUB), :] * part))
        for s, z, v in vals:
            CS[s, pl.ds(z, SUB), :] = v
        return carry

    lax.fori_loop(0, p.NZ // step, weigh, 0)


def basis_kernel(plan, coup_any, recv, factor, size, C, CS, basis, sums, G, W, B, R0, BB, keep, own, coup, sem):
    p = plan
    nx, off, n = p.nx, SUB, p.depth
    move = pltpu.make_async_copy(coup_any, coup, sem)
    move.start()
    geo = Line(p)
    step = TILES * SUB
    geo.edges(G)
    geo.edges(W)

    def put(s, z, val):
        rows = pl.ds(z, SUB)
        B[0, s, rows, :] = val
        R0[s, rows, :] = val

    geo.spread(recv, put)
    move.wait()
    ki = [coup[0, k] for k in range(9)]
    ke = [coup[1, k] for k in range(9)]
    total = ki[0] + ke[0]
    for k in range(1, 9):
        total = total + (ki[k] + ke[k])
    quarter = 2.0 / (total * size[...])
    ki, ke = mixed(ki), mixed(ke)
    zero = jnp.zeros((SUB, nx), f32)
    lane_row = lax.broadcasted_iota(jnp.int32, (1, nx), 1)

    def vectors(j):
        cur = j % 3

        def split(s, carry):
            b = B[cur, s]
            high = b.astype(jnp.bfloat16)
            cols = pl.ds(pl.multiple_of(s * nx, nx), nx)
            BB[pl.ds(0, p.NZ), cols] = high
            BB[pl.ds(p.NZ, p.NZ), cols] = high
            BB[pl.ds(2 * p.NZ, p.NZ), cols] = (b - high.astype(f32)).astype(jnp.bfloat16)
            return carry

        lax.fori_loop(0, p.slabs, split, 0)
        prod = jnp.dot(factor[...], BB[...], preferred_element_type=f32)
        body = pl.ds(off, p.NZ)
        for s in range(p.slabs):
            part = prod[:, s * nx : (s + 1) * nx]
            basis[j, s] = part
            W[s + 1, body, :] = part
            G[s + 1, body, :] = part * C[s]
        geo.wrap(W)
        geo.wrap(G)

    def apply(j):
        cur, prev, new = j % 3, (j + 2) % 3, (j + 1) % 3
        last = j == n - 1
        gain_e = quarter if j else 0.5 * quarter

        def block(t, carry):
            accs = [list(c) for c in carry]
            stores = []
            for k in range(TILES):
                z = pl.multiple_of(t * step, step) + k * SUB
                rows = pl.ds(z, SUB)
                for s in range(p.slabs):
                    w = W[s + 1, pl.ds(off + z, SUB), :]
                    inner = combine(geo.tile_of(G, s, z), ki, None, None, nx)
                    outer = combine(geo.tile_of(W, s, z), ke, None, None, nx)
                    e = CS[s, rows, :] * w - C[s, rows, :] * inner - outer
                    e = e * keep[s]
                    if j == 0:
                        stores.append((s, rows, gain_e * e - B[cur, s, rows, :]))
                    elif not last:
                        stores.append((s, rows, gain_e * e - 2.0 * B[cur, s, rows, :] - B[prev, s, rows, :]))
                    e = e * own[s]
                    for i in range(j + 1):
                        v = w if i == j else basis[i, s, rows, :]
                        accs[i][k % 2] = accs[i][k % 2] + v * e
                    accs[j + 1][k % 2] = accs[j + 1][k % 2] + (w * own[s]) * R0[s, rows, :]
            for s, rows, value in stores:
                B[new, s, rows, :] = value
            return tuple(tuple(a) for a in accs)

        accs = lax.fori_loop(0, p.NZ // step, block, tuple((zero, zero) for _ in range(j + 2)))
        return [a + b for a, b in accs]

    def fill(out, acc, at):
        v = jnp.sum(jnp.sum(acc, axis=0, keepdims=True), axis=1, keepdims=True)
        return jnp.where(lane_row == at, v, out)

    for s in range(p.slabs):
        keep[s] = jnp.where(geo.inside(s), 1.0, 0.0)
        own[s] = jnp.where(geo.own(s), 1.0, 0.0)
    out = jnp.zeros((1, nx), f32)
    for j in range(n):
        vectors(j)
        accs = apply(j)
        out = fill(out, accs[j + 1], j)
        for i in range(j + 1):
            out = fill(out, accs[i], n + n * j + i)
    sums[...] = jnp.broadcast_to(out, sums.shape)


def solve_kernel(plan, recv, basis, send):
    p = plan
    nx, n = p.nx, p.depth
    tot = jnp.sum(recv[...], axis=0, keepdims=True)

    def get(k):
        return jnp.broadcast_to(tot[:, k : k + 1], (SUB, nx))

    rhs = [get(j) for j in range(n)]
    A = [[None] * n for _ in range(n)]
    for j in range(n):
        for i in range(j + 1):
            A[i][j] = A[j][i] = get(n + n * j + i)
    diag = [A[i][i] for i in range(n)]
    inv = [None] * n
    for k in range(n):
        ok = A[k][k] > 1e-7 * diag[k]
        inv[k] = jnp.where(ok, 1.0 / jnp.where(ok, A[k][k], 1.0), 0.0)
        for i in range(k + 1, n):
            m = A[i][k] * inv[k]
            for l in range(k + 1, n):
                A[i][l] = A[i][l] - m * A[k][l]
            rhs[i] = rhs[i] - m * rhs[k]
    sol = [None] * n
    for k in reversed(range(n)):
        acc = rhs[k]
        for l in range(k + 1, n):
            acc = acc - A[k][l] * sol[l]
        sol[k] = acc * inv[k]

    lane = lax.broadcasted_iota(jnp.int32, (SUB, nx), 1)
    group = lane // p.cols
    per = p.nz // SUB

    def pack(t, carry):
        rows = pl.ds(pl.multiple_of(t * SUB, SUB), SUB)
        dst = t // per
        part = []
        for s in range(p.slabs):
            acc = sol[0] * basis[0, s, rows, :]
            for i in range(1, n):
                acc = acc + sol[i] * basis[i, s, rows, :]
            part.append(acc)
        for o in range(p.back):
            acc = None
            for q2 in range(p.back_grp):
                y = p.depth + o * p.back_grp + q2
                q, s = y // p.slabs, y % p.slabs
                amount = (p.cols * q2 - (p.wid * q + p.hx)) % nx
                piece = pltpu.roll(part[s], amount, 1) if amount else part[s]
                acc = piece if acc is None else jnp.where(group == q2, piece, acc)
            send[dst, pl.ds(pl.multiple_of(o * p.nz + (t % per) * SUB, SUB), SUB), :] = acc
        return carry

    lax.fori_loop(0, p.NZ // SUB, pack, 0, unroll=2)


def finish_kernel(plan, recv, pot, out):
    p = plan
    nx = p.nx
    lane = lax.broadcasted_iota(jnp.int32, (SUB, nx), 1)
    group = lane // p.cols
    fpot = pot.reshape(p.nz * p.ny, nx)
    fout = out.reshape(p.nz * p.ny, nx)
    for o in range(p.back):
        for zt in range(p.nz // SUB):
            src = [recv[j, pl.ds(o * p.nz + zt * SUB, SUB), :] for j in range(p.ngx)]
            for q2 in range(p.back_grp):
                acc = None
                for j in range(p.ngx):
                    amount = (p.cols * j - p.cols * q2) % nx
                    piece = pltpu.roll(src[j], amount, 1) if amount else src[j]
                    acc = piece if acc is None else jnp.where(group == j, piece, acc)
                rows = pl.ds(zt * SUB * p.ny + o * p.back_grp + q2, SUB, stride=p.ny)
                fout[rows, :] = fpot[rows, :] + acc


def bidomain_step(voltage, potential, tissue, gain, couplings, line_factor):
    ngx, ngy = lax.axis_size("gx"), lax.axis_size("gy")
    p = Plan(voltage.shape, ngx, ngy)
    nz, ny, nx = p.nz, p.ny, p.nx
    sds = jax.ShapeDtypeStruct

    def call(kernel, ins, outs, scratch=(), mib=12):
        return pl.pallas_call(
            kernel,
            out_shape=outs,
            in_specs=ins,
            out_specs=[VMEM] * len(outs),
            scratch_shapes=list(scratch),
            compiler_params=pltpu.CompilerParams(vmem_limit_bytes=mib * 1024 * 1024),
        )

    ysends = [None] if p.swap else [1, -1]
    shapes, routes = [], []

    def pairs(dz, dy):
        res = []
        for a in range(ngx):
            for b in range(ngy):
                if dy is None:
                    tb = (b + 1) % 2
                else:
                    tb = b + dy
                if 0 <= a + dz < ngx and 0 <= tb < ngy:
                    res.append((a * ngy + b, (a + dz) * ngy + tb))
        return res

    for dy in ysends:
        shapes.append(sds((3, nz, p.hy, nx), f32))
        routes.append((0, dy))
    for hop, n in p.hops:
        for sign in (1, -1):
            shapes.append(sds((3, n, ny, nx), f32))
            routes.append((sign * hop, 0))
            for dy in ysends:
                shapes.append(sds((3, n, p.hy, nx), f32))
                routes.append((sign * hop, dy))

    volt, pot, cond, *pieces = call(
        lambda *a: prep_kernel(p, *a),
        [pl.BlockSpec(memory_space=pltpu.HBM)] * 4,
        [sds(voltage.shape, f32)] * 3 + shapes,
        [pltpu.VMEM(voltage.shape, jnp.int32), pltpu.VMEM(voltage.shape, f32), pltpu.SemaphoreType.DMA((4,))],
    )(*(pltpu.with_memory_space_constraint(x, pltpu.HBM) for x in (voltage, potential, tissue, gain)))
    halos = []
    for x, r in zip(pieces, routes):
        halos.append(lax.ppermute(x, ("gx", "gy"), pairs(*r)))

    line = pltpu.VMEM((p.slabs, p.NZ, nx), f32)
    flag = pltpu.VMEM((p.slabs, SUB, nx), f32)
    table = [pltpu.SMEM(couplings.shape, f32), pltpu.SemaphoreType.DMA]
    wide = pltpu.VMEM((p.slabs + 2, p.NZ + 2 * SUB, nx), f32)
    half = pltpu.VMEM((3 * p.NZ, p.slabs * nx), jnp.bfloat16)

    def swap_lines(x):
        return lax.all_to_all(x, "gx", split_axis=0, concat_axis=0, tiled=True)

    sides = halos[: len(ysends)]
    (send_c,) = call(
        lambda *a: cond_kernel(p, *a), [VMEM] * (1 + len(sides)), [sds((ngx, p.slabs * nz, nx), f32)]
    )(cond, *sides)
    recv_c = swap_lines(send_c)
    line_c, line_cs = call(
        lambda *a: line_kernel(p, *a),
        [ANY, VMEM],
        [sds((p.slabs, p.NZ, nx), f32)] * 2,
        [wide] + table,
    )(couplings, recv_c)

    n_line = line_factor.shape[0]
    parts, size = call(
        factor_kernel, [VMEM] * 2, [sds((n_line, 3 * n_line), jnp.bfloat16), sds((SUB, nx), f32)]
    )(line_factor, line_factor.T)

    ext = pltpu.VMEM((p.yrows, p.zrows, nx), f32)
    new_voltage, send = call(
        lambda *a: cheb_kernel(p, *a),
        [ANY] + [VMEM] * (3 + len(halos)),
        [sds(voltage.shape, f32), sds((ngx, p.slabs * nz, nx), f32)],
        [ext] * 9 + table,
        mib=24,
    )(couplings, volt, pot, cond, *halos)

    recv = swap_lines(send)
    basis, sums = call(
        lambda *a: basis_kernel(p, *a),
        [ANY] + [VMEM] * 5,
        [sds((p.depth, p.slabs, p.NZ, nx), f32), sds((ngx * ngy, nx), f32)],
        [wide, wide, pltpu.VMEM((3, p.slabs, p.NZ, nx), f32), line, half, flag, flag] + table,
        mib=24,
    )(couplings, recv, parts, size, line_c, line_cs)

    shares = lax.all_to_all(
        sums.reshape(ngx * ngy, 1, nx), ("gx", "gy"), split_axis=0, concat_axis=0, tiled=True
    ).reshape(ngx * ngy, nx)

    (back,) = call(
        lambda *a: solve_kernel(p, *a), [VMEM] * 2, [sds((ngx, p.back * nz, nx), f32)]
    )(shares, basis)
    home = lax.all_to_all(back, "gx", split_axis=0, concat_axis=0, tiled=True)
    (new_potential,) = call(
        lambda *a: finish_kernel(p, *a), [VMEM] * 2, [sds(voltage.shape, f32)]
    )(home, pot)
    return new_voltage, new_potential


def solution(mesh):
    spec = P("gx", "gy", None)
    return jax.shard_map(
        bidomain_step,
        mesh=mesh,
        in_specs=(spec, spec, spec, spec, P(), P()),
        out_specs=(spec, spec),
        check_vma=False,
    )
```

```python
import jax
import jax.numpy as jnp
from jax import lax
from jax.experimental import pallas as pl
from jax.experimental.pallas import tpu as pltpu
from jax.sharding import PartitionSpec as P


CHEB = 8
ITERS = 4
SUB = 8
TRIP = 48
TILES = 8

time_step = 2.0
ionic_rate = 0.5
onset_level = 0.2
gain_top = 3.0625
f32 = jnp.float32
VMEM = pl.BlockSpec(memory_space=pltpu.VMEM)
ANY = pl.BlockSpec(memory_space=pl.ANY)


def up_to(n, m):
    return -(-n // m) * m


class Plan:
    def __init__(self, local_shape, ngx, ngy):
        self.nz, self.ny, self.nx = local_shape
        self.ngx, self.ngy = ngx, ngy
        self.depth = ITERS
        self.hz = CHEB + 1
        self.hy = up_to(CHEB + 1 + ITERS, SUB)
        self.swap = ngy == 2
        self.hops = []
        left, hop = self.hz, 1
        while left > 0:
            self.hops.append((hop, min(self.nz, left)))
            left -= self.nz
            hop += 1
        self.pad = up_to(ITERS + 1, SUB)
        self.ywin = self.ny + self.hy * (1 if self.swap else 2)
        self.yrows = self.ywin + 2 * self.pad
        self.zrows = up_to(max(self.hz - d + up_to(self.nz + 2 * d, SUB) + 1 for d in range(self.hz)), SUB)
        self.zrows = max(self.zrows, up_to(self.nz + 2 * self.hz, SUB))
        self.NZ = self.nz * ngx
        self.cols = self.nx // ngx
        self.wid = 1
        while self.wid < self.cols + 2 * self.depth:
            self.wid *= 2
        self.hx = (self.wid - self.cols) // 2
        self.grp = self.nx // self.wid
        self.inner = self.ny // self.grp
        self.slabs = -(-(self.ny + 2 * self.depth) // self.grp)
        self.back_grp = self.nx // self.cols
        self.back = self.ny // self.back_grp


def here():
    return lax.axis_index("gx"), lax.axis_index("gy")


def block_rows(count, tiles):
    def cost(r):
        trips = -(-count // r)
        return trips * (150 + 9 * r * tiles) if trips * r - count < SUB - 1 else 1 << 30

    return min(range(1, max(2, TRIP // tiles + 1)), key=cost)


def prep_kernel(plan, volt_hbm, pot_hbm, tissue_hbm, gain_hbm, volt, pot, cond, *rest):
    *outs, tissue, gain, sems = rest
    idx = here()
    moves = [
        pltpu.make_async_copy(src, dst, sems.at[i])
        for i, (src, dst) in enumerate(
            ((tissue_hbm, tissue), (gain_hbm, gain), (volt_hbm, volt), (pot_hbm, pot))
        )
    ]
    for move in moves:
        move.start()
    moves[0].wait()
    moves[1].wait()
    cond[...] = tissue[...].astype(f32) * gain[...]
    moves[2].wait()
    moves[3].wait()
    fields = (volt, pot, cond)
    if plan.swap:
        ys = [pl.multiple_of((1 - idx[1]) * (plan.ny - plan.hy), SUB)]
    else:
        ys = [plan.ny - plan.hy, 0]
    at = 0
    for y0 in ys:
        for f, ref in enumerate(fields):
            outs[at][f] = ref[:, pl.ds(y0, plan.hy), :]
        at += 1
    for _, n in plan.hops:
        for z0 in (plan.nz - n, 0):
            for f, ref in enumerate(fields):
                outs[at][f] = ref[pl.ds(z0, n)]
            at += 1
            for y0 in ys:
                for f, ref in enumerate(fields):
                    outs[at][f] = ref[pl.ds(z0, n), pl.ds(y0, plan.hy), :]
                at += 1


def mixed(k):
    k = list(k)
    return k[:5] + [0.5 * (k[5] + k[6]), 0.5 * (k[5] - k[6]), 0.5 * (k[7] + k[8]), 0.5 * (k[7] - k[8])]


def combine(tile, k, left, right, width):
    mid, zp, zm, yp, ym = tile(0, 0), tile(1, 0), tile(-1, 0), tile(0, 1), tile(0, -1)
    zpyp, zmym, zpym, zmyp = tile(1, 1), tile(-1, -1), tile(1, -1), tile(-1, 1)
    zs, ys = zp + zm, yp + ym
    same = (k[0] * zs + k[1] * ys) + (k[3] * (zpyp + zmym) + k[4] * (zpym + zmyp))
    even = k[2] * mid + (k[5] * zs + k[7] * ys)
    odd = k[6] * (zp - zm) + k[8] * (yp - ym)
    plus = pltpu.roll(even + odd, width - 1, 1)
    minus = pltpu.roll(even - odd, 1, 1)
    if left is not None:
        plus = jnp.where(right, 0.0, plus)
        minus = jnp.where(left, 0.0, minus)
    return same + (plus + minus)


def cheb_kernel(plan, coup_any, volt, pot, cond, *rest):
    p = plan
    idx = here()
    ny_halo = 1 if p.swap else 2
    n_in = ny_halo + len(p.hops) * 2 * (1 + ny_halo)
    halos = rest[:n_in]
    new_volt, send = rest[n_in : n_in + 2]
    C, G0, G1, E, PT, R, U, D, C2, coup, sem = rest[n_in + 2 :]
    move = pltpu.make_async_copy(coup_any, coup, sem)
    move.start()
    nx = p.nx
    flat = lambda ref: ref.reshape(p.yrows * p.zrows, nx)
    if p.swap:
        ylocal = p.pad + idx[1] * p.hy
        yhalo = [p.pad + (1 - idx[1]) * p.ny]
    else:
        ylocal = p.pad + p.hy
        yhalo = [p.pad, p.pad + p.hy + p.ny]

    zero_rows = jnp.zeros((p.pad, p.zrows, nx), f32)
    for ref in (C, G0, G1, E, PT, R, U, D, C2):
        ref[pl.ds(0, p.pad)] = zero_rows
        ref[pl.ds(p.pad + p.ywin, p.pad)] = zero_rows

    fc, fg, fe, fp, fr = (flat(r) for r in (C, G0, E, PT, R))

    def place(getter, planes, zrow0, yrow0, ycount):
        def one(z, carry):
            for t in range(ycount // SUB):
                v, q, c = getter(z, t)
                start = (yrow0 + t * SUB) * p.zrows + zrow0 + z
                rows = pl.ds(start, SUB, stride=p.zrows)
                s = v + q
                mask = jnp.where(c > 0.0, 1.0, 0.0)
                fc[rows, :] = c
                fg[rows, :] = c * s
                fe[rows, :] = s
                fp[rows, :] = q
                fr[rows, :] = (-ionic_rate) * mask * v * (v - onset_level) * (v - 1.0)
            return carry

        lax.fori_loop(0, planes, one, 0)

    def local(z, t):
        ys = pl.ds(t * SUB, SUB)
        return volt[z, ys, :], pot[z, ys, :], cond[z, ys, :]

    def piece(ref):
        def get(z, t):
            ys = pl.ds(t * SUB, SUB)
            return ref[0, z, ys, :], ref[1, z, ys, :], ref[2, z, ys, :]

        return get

    place(local, p.nz, p.hz, ylocal, p.ny)
    at = 0
    for y0 in yhalo:
        place(piece(halos[at]), p.nz, p.hz, y0, p.hy)
        at += 1
    done = 0
    for _, n in p.hops:
        for z0 in (p.hz - done - n, p.hz + p.nz + done):
            place(piece(halos[at]), n, z0, ylocal, p.ny)
            at += 1
            for y0 in yhalo:
                place(piece(halos[at]), n, z0, y0, p.hy)
                at += 1
        done += n

    lane = lax.broadcasted_iota(jnp.int32, (SUB, nx), 1)
    left, right = lane == 0, lane == nx - 1
    move.wait()
    ki = [coup[0, k] for k in range(9)]
    ke = [coup[1, k] for k in range(9)]
    total, ke_sum = ki[0], ke[0]
    for k in range(1, 9):
        total = total + ki[k]
        ke_sum = ke_sum + ke[k]
    ke_sum = 2.0 * ke_sum
    ki, ke = mixed(ki), mixed(ke)
    top = 1.0 + time_step * 4.0 * gain_top * jnp.full((SUB, nx), total, f32)
    centre = (top + 1.0) / 2.0
    half = (top - 1.0) / 2.0
    ratio = centre / half
    weight = 1.0 / ratio
    inv_centre = 1.0 / centre

    def sweep(d, body):
        tiles = up_to(p.nz + 2 * d, SUB) // SUB
        over = p.hy - p.depth - d
        y0 = p.pad + (idx[1] * over if p.swap else over)
        count = p.ny + (d + p.depth) * (1 if p.swap else 2)

        step = block_rows(count, tiles)

        def block(i, carry):
            stores = []
            for r in range(step):
                for t in range(tiles):
                    stores += body(y0 + i * step + r, p.hz - d + t * SUB)
            for ref, where, value in stores:
                ref[where] = value
            return carry

        lax.fori_loop(0, -(-count // step), block, 0)

    def tile_of(ref, y, z):
        return lambda dz, dy: ref[y + dy, pl.ds(z + dz, SUB), :]

    def first(y, z):
        rows = pl.ds(z, SUB)
        c = C[y, rows, :]
        s = E[y, rows, :]
        c2 = time_step * c
        cs = c2 * combine(tile_of(C, y, z), ki, left, right, nx)
        r = R[y, rows, :] - (cs * s - c2 * combine(tile_of(G0, y, z), ki, left, right, nx))
        u = r * inv_centre
        at = (y, rows)
        return [(D, at, 1.0 + cs), (C2, at, c2), (R, at, r), (U, at, u), (E, at, s + u), (G1, at, c * u)]

    sweep(CHEB, first)
    bufs = [G0, G1]
    for k in range(1, CHEB):
        gin, gout = bufs[k % 2], bufs[(k + 1) % 2]
        nxt = 1.0 / (2.0 * ratio - weight)
        keep, add = nxt * weight, 2.0 * nxt / half
        weight = nxt
        last = k == CHEB - 1

        def step(y, z, gin=gin, gout=gout, keep=keep, add=add, last=last):
            rows = pl.ds(z, SUB)
            c = C[y, rows, :]
            u = U[y, rows, :]
            flow = D[y, rows, :] * u - C2[y, rows, :] * combine(tile_of(gin, y, z), ki, left, right, nx)
            r = R[y, rows, :] - flow
            u = keep * u + add * r
            e = E[y, rows, :] + u
            at = (y, rows)
            if last:
                return [(E, at, e), (gout, at, c * e)]
            return [(E, at, e), (R, at, r), (U, at, u), (gout, at, c * u)]

        sweep(CHEB - k, step)

    gin = bufs[CHEB % 2]

    def final(y, z):
        rows = pl.ds(z, SUB)
        e = E[y, rows, :]
        flow = (D[y, rows, :] - 1.0) * e - C2[y, rows, :] * combine(tile_of(gin, y, z), ki, left, right, nx)
        outer = ke_sum * PT[y, rows, :] - combine(tile_of(PT, y, z), ke, left, right, nx)
        return [(R, (y, rows), (-1.0 / time_step) * flow - outer)]

    sweep(0, final)

    def give(z, carry):
        for t in range(p.ny // SUB):
            start = (ylocal + t * SUB) * p.zrows + p.hz + z
            rows = pl.ds(start, SUB, stride=p.zrows)
            new_volt[z, pl.ds(t * SUB, SUB), :] = fe[rows, :] - fp[rows, :]
        return carry

    lax.fori_loop(0, p.nz, give, 0)

    first_row = ylocal - p.depth

    def pack(s, carry):
        for zt in range(p.nz // SUB):
            rows = pl.ds(p.hz + zt * SUB, SUB)
            src = [R[first_row + q * p.slabs + s, rows, :] for q in range(p.grp)]
            windows(p, src, send, pl.multiple_of(s * p.nz + zt * SUB, SUB))
        return carry

    lax.fori_loop(0, p.slabs, pack, 0)


def windows(p, src, send, row):
    group = lax.broadcasted_iota(jnp.int32, (SUB, p.nx), 1) // p.wid
    for j in range(p.ngx):
        acc = None
        for q in range(p.grp):
            amount = (p.wid * q - (p.cols * j - p.hx)) % p.nx
            part = pltpu.roll(src[q], amount, 1) if amount else src[q]
            acc = part if acc is None else jnp.where(group == q, part, acc)
        send[j, pl.ds(row, SUB), :] = acc


def cond_kernel(plan, cond, send):
    p = plan
    flat = cond.reshape(p.nz * p.ny, p.nx)
    for s in range(p.inner):
        for zt in range(p.nz // SUB):
            src = [flat[pl.ds(zt * SUB * p.ny + q * p.inner + s, SUB, stride=p.ny), :] for q in range(p.grp)]
            windows(p, src, send, s * p.nz + zt * SUB)


def edge_kernel(plan, recv, *outs):
    p = plan
    idx = here()
    group = lax.broadcasted_iota(jnp.int32, (SUB, p.nx), 1) // p.wid
    per = p.nz // SUB

    def pick(t, y0):
        acc = jnp.zeros((SUB, p.nx), f32)
        for i in range(p.depth):
            q, s = (y0 + i) // p.inner, (y0 + i) % p.inner
            amount = (p.wid * (i - q)) % p.nx
            part = recv[t // per, pl.ds(pl.multiple_of(s * p.nz + (t % per) * SUB, SUB), SUB), :]
            part = pltpu.roll(part, amount, 1) if amount else part
            acc = jnp.where(group == i, part, acc)
        return acc

    def one(t, carry):
        rows = pl.ds(pl.multiple_of(t * SUB, SUB), SUB)
        head, tail = pick(t, 0), pick(t, p.ny - p.depth)
        if p.swap:
            outs[0][rows, :] = jnp.where(idx[1] == 0, tail, head)
        else:
            outs[0][rows, :] = tail
            outs[1][rows, :] = head
        return carry

    lax.fori_loop(0, p.NZ // SUB, one, 0, unroll=4)


def factor_kernel(line, line_t, parts, size):
    scale = 1.0 / jnp.max(jnp.abs(line[...]), keepdims=True)
    a = line_t[...] * scale
    b = line[...] * scale
    g = jnp.dot(a, b, precision=lax.Precision.HIGHEST, preferred_element_type=f32)
    high = g.astype(jnp.bfloat16)
    n = g.shape[0]
    parts[:, pl.ds(0, n)] = high
    parts[:, pl.ds(n, n)] = (g - high.astype(f32)).astype(jnp.bfloat16)
    parts[:, pl.ds(2 * n, n)] = high

    def norm(m):
        return jnp.sqrt(jnp.sum(jnp.sum(m * m, axis=0, keepdims=True), axis=1, keepdims=True))

    n = norm(g)
    est = n
    m = g / n
    for power in range(3):
        mb = m.astype(jnp.bfloat16)
        m = jnp.dot(mb, mb, preferred_element_type=f32)
        n = norm(m)
        m = m / n
        root = n
        for _ in range(power + 1):
            root = jnp.sqrt(root)
        est = est * root
    size[...] = jnp.broadcast_to(est, size.shape)


class Line:
    def __init__(self, p):
        idx = here()
        self.p = p
        self.lane = lax.broadcasted_iota(jnp.int32, (SUB, p.nx), 1)
        self.idx = idx
        x = p.cols * idx[0] - p.hx + self.lane % p.wid
        self.xin = (x >= 0) & (x < p.nx)
        self.xown = (self.lane % p.wid >= p.hx) & (self.lane % p.wid < p.hx + p.cols)

    def ywin(self, s):
        return (self.lane // self.p.wid) * self.p.slabs + s

    def inside(self, s):
        p = self.p
        y = p.ny * self.idx[1] - p.depth + self.ywin(s)
        return self.xin & (y >= 0) & (y < p.ny * p.ngy)

    def own(self, s):
        p = self.p
        return self.xown & (self.ywin(s) >= p.depth) & (self.ywin(s) < p.depth + p.ny)

    def edges(self, ref):
        p = self.p
        for s in range(p.slabs + 2):
            ref[s, pl.ds(0, SUB), :] = jnp.zeros((SUB, p.nx), f32)
            ref[s, pl.ds(SUB + p.NZ, SUB), :] = jnp.zeros((SUB, p.nx), f32)

    def wrap(self, ref):
        p = self.p
        rows = pl.ds(SUB, p.NZ)
        ref[0, rows, :] = pltpu.roll(ref[p.slabs, rows, :], p.wid, 1)
        ref[p.slabs + 1, rows, :] = pltpu.roll(ref[1, rows, :], p.nx - p.wid, 1)

    def spread(self, recv, put):
        p = self.p

        def one(s, carry):
            keep = self.inside(s)
            for j in range(p.ngx):
                for zt in range(p.nz // SUB):
                    got = recv[j, pl.ds(pl.multiple_of(s * p.nz, SUB) + zt * SUB, SUB), :]
                    put(s, j * p.nz + zt * SUB, jnp.where(keep, got, 0.0))
            return carry

        lax.fori_loop(0, p.slabs, one, 0)

    def tile_of(self, ref, s, z):
        return lambda dz, dy: ref[s + 1 + dy, pl.ds(SUB + z + dz, SUB), :]


def line_kernel(plan, coup_any, recv, *rest):
    p = plan
    *edges, C, CS, G, coup, sem = rest
    nx = p.nx
    move = pltpu.make_async_copy(coup_any, coup, sem)
    move.start()
    geo = Line(p)
    geo.edges(G)
    group = geo.lane // p.wid
    per = p.nz // SUB
    masks = [geo.inside(s) for s in range(p.slabs)]

    def arrange(t, carry):
        z = pl.multiple_of(t * SUB, SUB)
        src = [
            recv[t // per, pl.ds(pl.multiple_of(s * p.nz + (t % per) * SUB, SUB), SUB), :] for s in range(p.inner)
        ]
        low, high = edges[0][pl.ds(z, SUB), :], edges[-1][pl.ds(z, SUB), :]
        vals = []
        for s in range(p.slabs):
            acc = jnp.zeros((SUB, nx), f32)
            for q in range(p.grp):
                y = q * p.slabs + s - p.depth
                if y < 0:
                    part, at = low, y + p.depth
                elif y < p.ny:
                    part, at = src[y % p.inner], y // p.inner
                elif y < p.ny + p.depth:
                    part, at = high, y - p.ny
                else:
                    continue
                amount = (p.wid * (q - at)) % nx
                part = pltpu.roll(part, amount, 1) if amount else part
                acc = jnp.where(group == q, part, acc)
            vals.append(jnp.where(masks[s], acc, 0.0))
        for s, val in enumerate(vals):
            C[s, pl.ds(z, SUB), :] = val
            G[s + 1, pl.ds(SUB + z, SUB), :] = val
        return carry

    lax.fori_loop(0, p.NZ // SUB, arrange, 0)
    geo.wrap(G)
    move.wait()
    ki = mixed([coup[0, k] for k in range(9)])
    ke_sum = coup[1, 0]
    for k in range(1, 9):
        ke_sum = ke_sum + coup[1, k]
    ke_twice = 2.0 * ke_sum
    step = TILES * SUB

    def weigh(t, carry):
        vals = []
        for k in range(TILES):
            z = pl.multiple_of(t * step, step) + k * SUB
            for s in range(p.slabs):
                part = combine(geo.tile_of(G, s, z), ki, None, None, nx)
                vals.append((s, z, ke_twice + C[s, pl.ds(z, SUB), :] * part))
        for s, z, v in vals:
            CS[s, pl.ds(z, SUB), :] = v
        return carry

    lax.fori_loop(0, p.NZ // step, weigh, 0)


def basis_kernel(plan, coup_any, recv, factor, size, C, CS, basis, sums, G, W, B, R0, BB, keep, own, coup, sem):
    p = plan
    nx, off, n = p.nx, SUB, p.depth
    move = pltpu.make_async_copy(coup_any, coup, sem)
    move.start()
    geo = Line(p)
    step = TILES * SUB
    geo.edges(G)
    geo.edges(W)

    def put(s, z, val):
        rows = pl.ds(z, SUB)
        B[0, s, rows, :] = val
        R0[s, rows, :] = val

    geo.spread(recv, put)
    move.wait()
    ki = [coup[0, k] for k in range(9)]
    ke = [coup[1, k] for k in range(9)]
    total = ki[0] + ke[0]
    for k in range(1, 9):
        total = total + (ki[k] + ke[k])
    quarter = 2.0 / (total * size[...])
    ki, ke = mixed(ki), mixed(ke)
    zero = jnp.zeros((SUB, nx), f32)
    lane_row = lax.broadcasted_iota(jnp.int32, (1, nx), 1)

    def vectors(j):
        cur = j % 3

        def split(s, carry):
            b = B[cur, s]
            high = b.astype(jnp.bfloat16)
            cols = pl.ds(pl.multiple_of(s * nx, nx), nx)
            BB[pl.ds(0, p.NZ), cols] = high
            BB[pl.ds(p.NZ, p.NZ), cols] = high
            BB[pl.ds(2 * p.NZ, p.NZ), cols] = (b - high.astype(f32)).astype(jnp.bfloat16)
            return carry

        lax.fori_loop(0, p.slabs, split, 0)
        prod = jnp.dot(factor[...], BB[...], preferred_element_type=f32)
        body = pl.ds(off, p.NZ)
        for s in range(p.slabs):
            part = prod[:, s * nx : (s + 1) * nx]
            basis[j, s] = part
            W[s + 1, body, :] = part
            G[s + 1, body, :] = part * C[s]
        geo.wrap(W)
        geo.wrap(G)

    def apply(j):
        cur, prev, new = j % 3, (j + 2) % 3, (j + 1) % 3
        last = j == n - 1
        gain_e = quarter if j else 0.5 * quarter

        def block(t, carry):
            accs = [list(c) for c in carry]
            stores = []
            for k in range(TILES):
                z = pl.multiple_of(t * step, step) + k * SUB
                rows = pl.ds(z, SUB)
                for s in range(p.slabs):
                    w = W[s + 1, pl.ds(off + z, SUB), :]
                    inner = combine(geo.tile_of(G, s, z), ki, None, None, nx)
                    outer = combine(geo.tile_of(W, s, z), ke, None, None, nx)
                    e = CS[s, rows, :] * w - C[s, rows, :] * inner - outer
                    e = e * keep[s]
                    if j == 0:
                        stores.append((s, rows, gain_e * e - B[cur, s, rows, :]))
                    elif not last:
                        stores.append((s, rows, gain_e * e - 2.0 * B[cur, s, rows, :] - B[prev, s, rows, :]))
                    e = e * own[s]
                    for i in range(j + 1):
                        v = w if i == j else basis[i, s, rows, :]
                        accs[i][k % 2] = accs[i][k % 2] + v * e
                    accs[j + 1][k % 2] = accs[j + 1][k % 2] + (w * own[s]) * R0[s, rows, :]
            for s, rows, value in stores:
                B[new, s, rows, :] = value
            return tuple(tuple(a) for a in accs)

        accs = lax.fori_loop(0, p.NZ // step, block, tuple((zero, zero) for _ in range(j + 2)))
        return [a + b for a, b in accs]

    def fill(out, acc, at):
        v = jnp.sum(jnp.sum(acc, axis=0, keepdims=True), axis=1, keepdims=True)
        return jnp.where(lane_row == at, v, out)

    for s in range(p.slabs):
        keep[s] = jnp.where(geo.inside(s), 1.0, 0.0)
        own[s] = jnp.where(geo.own(s), 1.0, 0.0)
    out = jnp.zeros((1, nx), f32)
    for j in range(n):
        vectors(j)
        accs = apply(j)
        out = fill(out, accs[j + 1], j)
        for i in range(j + 1):
            out = fill(out, accs[i], n + n * j + i)
    sums[...] = jnp.broadcast_to(out, sums.shape)


def solve_kernel(plan, recv, basis, send):
    p = plan
    nx, n = p.nx, p.depth
    tot = jnp.sum(recv[...], axis=0, keepdims=True)

    def get(k):
        return jnp.broadcast_to(tot[:, k : k + 1], (SUB, nx))

    rhs = [get(j) for j in range(n)]
    A = [[None] * n for _ in range(n)]
    for j in range(n):
        for i in range(j + 1):
            A[i][j] = A[j][i] = get(n + n * j + i)
    diag = [A[i][i] for i in range(n)]
    inv = [None] * n
    for k in range(n):
        ok = A[k][k] > 1e-7 * diag[k]
        inv[k] = jnp.where(ok, 1.0 / jnp.where(ok, A[k][k], 1.0), 0.0)
        for i in range(k + 1, n):
            m = A[i][k] * inv[k]
            for l in range(k + 1, n):
                A[i][l] = A[i][l] - m * A[k][l]
            rhs[i] = rhs[i] - m * rhs[k]
    sol = [None] * n
    for k in reversed(range(n)):
        acc = rhs[k]
        for l in range(k + 1, n):
            acc = acc - A[k][l] * sol[l]
        sol[k] = acc * inv[k]

    lane = lax.broadcasted_iota(jnp.int32, (SUB, nx), 1)
    group = lane // p.cols
    per = p.nz // SUB

    def pack(t, carry):
        rows = pl.ds(pl.multiple_of(t * SUB, SUB), SUB)
        dst = t // per
        part = []
        for s in range(p.slabs):
            acc = sol[0] * basis[0, s, rows, :]
            for i in range(1, n):
                acc = acc + sol[i] * basis[i, s, rows, :]
            part.append(acc)
        for o in range(p.back):
            acc = None
            for q2 in range(p.back_grp):
                y = p.depth + o * p.back_grp + q2
                q, s = y // p.slabs, y % p.slabs
                amount = (p.cols * q2 - (p.wid * q + p.hx)) % nx
                piece = pltpu.roll(part[s], amount, 1) if amount else part[s]
                acc = piece if acc is None else jnp.where(group == q2, piece, acc)
            send[dst, pl.ds(pl.multiple_of(o * p.nz + (t % per) * SUB, SUB), SUB), :] = acc
        return carry

    lax.fori_loop(0, p.NZ // SUB, pack, 0, unroll=2)


def finish_kernel(plan, recv, pot, out):
    p = plan
    nx = p.nx
    lane = lax.broadcasted_iota(jnp.int32, (SUB, nx), 1)
    group = lane // p.cols
    fpot = pot.reshape(p.nz * p.ny, nx)
    fout = out.reshape(p.nz * p.ny, nx)
    for o in range(p.back):
        for zt in range(p.nz // SUB):
            src = [recv[j, pl.ds(o * p.nz + zt * SUB, SUB), :] for j in range(p.ngx)]
            for q2 in range(p.back_grp):
                acc = None
                for j in range(p.ngx):
                    amount = (p.cols * j - p.cols * q2) % nx
                    piece = pltpu.roll(src[j], amount, 1) if amount else src[j]
                    acc = piece if acc is None else jnp.where(group == j, piece, acc)
                rows = pl.ds(zt * SUB * p.ny + o * p.back_grp + q2, SUB, stride=p.ny)
                fout[rows, :] = fpot[rows, :] + acc


def bidomain_step(voltage, potential, tissue, gain, couplings, line_factor):
    ngx, ngy = lax.axis_size("gx"), lax.axis_size("gy")
    p = Plan(voltage.shape, ngx, ngy)
    nz, ny, nx = p.nz, p.ny, p.nx
    sds = jax.ShapeDtypeStruct

    def call(kernel, ins, outs, scratch=(), mib=12):
        return pl.pallas_call(
            kernel,
            out_shape=outs,
            in_specs=ins,
            out_specs=[VMEM] * len(outs),
            scratch_shapes=list(scratch),
            compiler_params=pltpu.CompilerParams(vmem_limit_bytes=mib * 1024 * 1024),
        )

    ysends = [None] if p.swap else [1, -1]
    shapes, routes = [], []

    def pairs(dz, dy):
        res = []
        for a in range(ngx):
            for b in range(ngy):
                if dy is None:
                    tb = (b + 1) % 2
                else:
                    tb = b + dy
                if 0 <= a + dz < ngx and 0 <= tb < ngy:
                    res.append((a * ngy + b, (a + dz) * ngy + tb))
        return res

    for dy in ysends:
        shapes.append(sds((3, nz, p.hy, nx), f32))
        routes.append((0, dy))
    for hop, n in p.hops:
        for sign in (1, -1):
            shapes.append(sds((3, n, ny, nx), f32))
            routes.append((sign * hop, 0))
            for dy in ysends:
                shapes.append(sds((3, n, p.hy, nx), f32))
                routes.append((sign * hop, dy))

    volt, pot, cond, *pieces = call(
        lambda *a: prep_kernel(p, *a),
        [pl.BlockSpec(memory_space=pltpu.HBM)] * 4,
        [sds(voltage.shape, f32)] * 3 + shapes,
        [pltpu.VMEM(voltage.shape, jnp.int32), pltpu.VMEM(voltage.shape, f32), pltpu.SemaphoreType.DMA((4,))],
    )(*(pltpu.with_memory_space_constraint(x, pltpu.HBM) for x in (voltage, potential, tissue, gain)))
    halos = []
    for x, r in zip(pieces, routes):
        halos.append(lax.ppermute(x, ("gx", "gy"), pairs(*r)))

    line = pltpu.VMEM((p.slabs, p.NZ, nx), f32)
    flag = pltpu.VMEM((p.slabs, SUB, nx), f32)
    table = [pltpu.SMEM(couplings.shape, f32), pltpu.SemaphoreType.DMA]
    wide = pltpu.VMEM((p.slabs + 2, p.NZ + 2 * SUB, nx), f32)
    half = pltpu.VMEM((3 * p.NZ, p.slabs * nx), jnp.bfloat16)

    def swap_lines(x):
        return lax.all_to_all(x, "gx", split_axis=0, concat_axis=0, tiled=True)

    (send_c,) = call(lambda *a: cond_kernel(p, *a), [VMEM], [sds((ngx, p.inner * nz, nx), f32)])(cond)
    recv_c = swap_lines(send_c)
    edges = call(lambda *a: edge_kernel(p, *a), [VMEM], [sds((p.NZ, nx), f32)] * len(ysends))(recv_c)
    edges = [lax.ppermute(x, ("gx", "gy"), pairs(0, dy)) for x, dy in zip(edges, ysends)]
    line_c, line_cs = call(
        lambda *a: line_kernel(p, *a),
        [ANY] + [VMEM] * (1 + len(edges)),
        [sds((p.slabs, p.NZ, nx), f32)] * 2,
        [wide] + table,
    )(couplings, recv_c, *edges)

    n_line = line_factor.shape[0]
    parts, size = call(
        factor_kernel, [VMEM] * 2, [sds((n_line, 3 * n_line), jnp.bfloat16), sds((SUB, nx), f32)]
    )(line_factor, line_factor.T)

    ext = pltpu.VMEM((p.yrows, p.zrows, nx), f32)
    new_voltage, send = call(
        lambda *a: cheb_kernel(p, *a),
        [ANY] + [VMEM] * (3 + len(halos)),
        [sds(voltage.shape, f32), sds((ngx, p.slabs * nz, nx), f32)],
        [ext] * 9 + table,
        mib=24,
    )(couplings, volt, pot, cond, *halos)

    recv = swap_lines(send)
    basis, sums = call(
        lambda *a: basis_kernel(p, *a),
        [ANY] + [VMEM] * 5,
        [sds((p.depth, p.slabs, p.NZ, nx), f32), sds((ngx * ngy, nx), f32)],
        [wide, wide, pltpu.VMEM((3, p.slabs, p.NZ, nx), f32), line, half, flag, flag] + table,
        mib=24,
    )(couplings, recv, parts, size, line_c, line_cs)

    shares = lax.all_to_all(
        sums.reshape(ngx * ngy, 1, nx), ("gx", "gy"), split_axis=0, concat_axis=0, tiled=True
    ).reshape(ngx * ngy, nx)

    (back,) = call(
        lambda *a: solve_kernel(p, *a), [VMEM] * 2, [sds((ngx, p.back * nz, nx), f32)]
    )(shares, basis)
    home = lax.all_to_all(back, "gx", split_axis=0, concat_axis=0, tiled=True)
    (new_potential,) = call(
        lambda *a: finish_kernel(p, *a), [VMEM] * 2, [sds(voltage.shape, f32)]
    )(home, pot)
    return new_voltage, new_potential


def solution(mesh):
    spec = P("gx", "gy", None)
    return jax.shard_map(
        bidomain_step,
        mesh=mesh,
        in_specs=(spec, spec, spec, spec, P(), P()),
        out_specs=(spec, spec),
        check_vma=False,
    )
```
